32 devices in a mesh: grp: 4 (over y, core), blk: 8 (over z, x).
Axes of the slice: x: 2, y: 2, z: 4, core: 2. Of those that a mesh axis runs over, the one named last changes fastest.
Arguments:
- primal: float32 [262144], P(('blk', 'grp')), may hold values from -3 to 3
- dual: float32 [131072], P(('blk', 'grp')), may hold values from -3 to 3
- objective: float32 [262144], P(('blk', 'grp')), may hold values from -6 to 6
- lower: float32 [262144], P(('blk', 'grp')), may hold values from -2 to -0.5
- upper: float32 [262144], P(('blk', 'grp')), may hold values from 0.5 to 2
- bound_kind: int32 [262144], P(('blk', 'grp')), may hold values from 0 to 3
- rhs: float32 [131072], P(('blk', 'grp')), may hold values from -6 to 6
- row_kind: int32 [131072], P(('blk', 'grp')), may hold values 0 or 1
- q_tiles: float32 [4, 32, 512, 512], P('grp', 'blk'), may hold values from -0.25 to 0.25
- q_index: int32 [4, 2, 32], P('grp', None, 'blk'), may hold values from 0 to 127
- k_tiles: float32 [4, 48, 512, 512], P('grp', 'blk'), may hold values from -0.25 to 0.25
- k_rows: int32 [4, 48], P('grp', 'blk'), may hold values from 0 to 31
- k_cols: int32 [4, 48], P('grp', 'blk'), may hold values from 0 to 127
Outputs:
- final_primal: float32 [262144], P(('blk', 'grp'))
- final_dual: float32 [131072], P(('blk', 'grp'))
- primal_weight: float32 [], replicated
The draws below stay inside these ranges and needn't reach their ends.
Inputs may be any that keep to these rules, and one draw needn't show every extreme that they name: `q_index`: row and column tile indices of Hessian tiles, within the column group. `k_rows`: row tile within the tile's dual block. `bound_kind`: 0 free, 1 lower bound only, 2 both bounds, 3 upper bound only.
All inputs are finite; a program needn't handle non-finite values. No bound on the sum of `row_kind` on one device may be relied on, other than what follows from the above.
Results may differ from the reference program's by a relative error of at most 0.00017.
Values sent between devices are 32-bit elements; how exact they have to be, the bound alone decides.
A program may use at most 64 MiB of HBM per device.

```python
import jax
import jax.numpy as jnp
from jax import lax

TILE = 512
X_DEV = 8192
Y_DEV = 4096
KT = 6
ITERS = 2
NX = 262144
M = 131072
GT_COUNT = 128
RT = 32
QTILES = 32
KTILES = 48
N_GRP = 4
N_BLK = 8


def place_ends(result, rng, smallest, top_value):
    dims = result.shape
    place = [jax.random.randint(jax.random.fold_in(rng, axis), (), 0, dims[axis]) for axis in range(len(dims))]
    result = result.at[tuple(place)].set(smallest)
    longest = dims.index(max(dims))
    place[longest] = (place[longest] + 1) % dims[longest]
    return result.at[tuple(place)].set(top_value)


def steps_of(key, extent, split, low, largest):
    def one(axis_at, blocks):
        draws = jax.random.uniform(jax.random.fold_in(jax.random.fold_in(key, 6), axis_at), (blocks,), jnp.float32, low / len(split), largest / len(split))
        return jnp.repeat(jnp.exp(draws), extent[axis_at] // blocks).reshape((-1,) + (1,) * (len(extent) - axis_at - 1))

    gain = one(*split[0])
    for cut in split[1:]:
        gain = gain * one(*cut)
    return gain


def scatter_about(key, shape, spread, reach, cuts=(), kind=jnp.bfloat16):
    result = spread * jax.random.normal(key, shape, jnp.float32)
    if cuts:
        result = result * steps_of(key, shape, cuts, -0.22, 0.18)
    return jnp.clip(result, -reach, reach).astype(kind)


def setup_inputs(seed: int = 0) -> dict:
    keys = jax.random.split(jax.random.key(seed), 14)
    return {
        "primal": scatter_about(keys[0], (NX,), 0.5, 3.0, ((0, 32),), jnp.float32),
        "dual": scatter_about(keys[1], (M,), 0.5, 3.0, ((0, 32),), jnp.float32),
        "objective": scatter_about(keys[2], (NX,), 1.0, 6.0, ((0, 32),), jnp.float32),
        "lower": jnp.clip(-2.0 + 1.5 * jax.random.uniform(keys[3], (NX,), jnp.float32) ** steps_of(keys[3], (NX,), ((0, 32),), -0.2, 0.2), -2.0, -0.5),
        "upper": jnp.clip(0.5 + 1.5 * jax.random.uniform(keys[4], (NX,), jnp.float32) ** steps_of(keys[4], (NX,), ((0, 32),), -0.2, 0.2), 0.5, 2.0),
        "bound_kind": place_ends(jax.random.randint(keys[5], (NX,), 0, 4), jax.random.fold_in(keys[5], 1), 0, 3).astype(jnp.int32),
        "rhs": scatter_about(keys[6], (M,), 1.0, 6.0, ((0, 32),), jnp.float32),
        "row_kind": place_ends((jax.random.randint(keys[7], (M,), 0, 2) < 1).astype(jnp.int32), jax.random.fold_in(keys[7], 1), 0, 1),
        "q_tiles": scatter_about(keys[8], (N_GRP, QTILES, TILE, TILE), TILE ** -0.5, 0.25, ((0, 4), (1, 8)), jnp.float32),
        "q_index": place_ends(jax.random.randint(keys[9], (N_GRP, 2, QTILES), 0, GT_COUNT), jax.random.fold_in(keys[9], 1), 0, GT_COUNT - 1).astype(jnp.int32),
        "k_tiles": scatter_about(keys[10], (N_GRP, KTILES, TILE, TILE), TILE ** -0.5, 0.25, ((0, 4), (1, 8)), jnp.float32),
        "k_rows": place_ends(jax.random.randint(keys[11], (N_GRP, KTILES), 0, RT), jax.random.fold_in(keys[11], 1), 0, RT - 1).astype(jnp.int32),
        "k_cols": place_ends(jax.random.randint(keys[12], (N_GRP, KTILES), 0, GT_COUNT), jax.random.fold_in(keys[12], 1), 0, GT_COUNT - 1).astype(jnp.int32),
    }


def apply_tiles(tiles, rows, cols, vec, count):
    pieces = vec.reshape(-1, TILE)[cols]
    product = jnp.einsum('tij,tj->ti', tiles, pieces, precision=lax.Precision.HIGHEST)
    return jnp.zeros((count, TILE), product.dtype).at[rows].add(product).reshape(-1)

def apply_transposed(tiles, rows, cols, vec, count):
    pieces = vec.reshape(-1, TILE)[rows]
    product = jnp.einsum('tij,ti->tj', tiles, pieces, precision=lax.Precision.HIGHEST)
    return jnp.zeros((count, TILE), product.dtype).at[cols].add(product).reshape(-1)

def project(values, lower, upper, bound_kind):
    values = jnp.where((bound_kind == 1) | (bound_kind == 2), jnp.maximum(values, lower), values)
    return jnp.where((bound_kind == 2) | (bound_kind == 3), jnp.minimum(values, upper), values)

def reference(primal, dual, objective, lower, upper, bound_kind, rhs, row_kind, q_tiles, q_index, k_tiles, k_rows, k_cols):
    group_tiles = N_BLK * X_DEV // TILE
    block_tiles = N_GRP * Y_DEV // TILE
    owner = (jnp.arange(N_BLK * KT) // KT).astype(jnp.int32)

    def group_vec(values, group):
        return values.reshape(N_BLK, N_GRP, X_DEV)[:, group, :].reshape(-1)

    def to_layout(parts):
        return jnp.stack([p.reshape(N_BLK, X_DEV) for p in parts], axis=1).reshape(-1)

    def forward(values):
        cons_prod = None
        parts = []
        for group in range(N_GRP):
            column_vec = group_vec(values, group)
            parts.append(apply_tiles(q_tiles[group], q_index[group, 0], q_index[group, 1], column_vec, group_tiles))
            term = apply_tiles(k_tiles[group], owner * block_tiles + k_rows[group], k_cols[group], column_vec, N_BLK * block_tiles)
            cons_prod = term if cons_prod is None else cons_prod + term
        return (cons_prod, to_layout(parts))

    def transposed(duals):
        parts = []
        for group in range(N_GRP):
            parts.append(apply_transposed(k_tiles[group], owner * block_tiles + k_rows[group], k_cols[group], duals, group_tiles))
        return to_layout(parts)
    weight = jnp.asarray(1.0, jnp.float32)
    current, duals = (primal, dual)
    cons_prod, hess_prod = forward(current)
    for step in range(ITERS):
        step_primal = 0.5 / weight
        step_dual = 0.5 * weight
        gradient = hess_prod + objective - transposed(duals)
        updated = project(current - step_primal * gradient, lower, upper, bound_kind)
        next_cons, next_hess = forward(updated)
        extrap = 2.0 * next_cons - cons_prod
        dual_new = duals + step_dual * (rhs - extrap)
        dual_new = jnp.where(row_kind == 1, jnp.maximum(dual_new, 0.0), dual_new)
        primal_sq = jnp.sum((updated - current) ** 2)
        dual_sq = jnp.sum((dual_new - duals) ** 2)
        weight = jnp.sqrt(weight * jnp.sqrt((dual_sq + 1e-06) / (primal_sq + 1e-06)))
        current, duals = (updated, dual_new)
        cons_prod, hess_prod = (next_cons, next_hess)
    return (current, duals, weight)
```

```python
import functools

import jax
import jax.numpy as jnp
from jax import lax
from jax.experimental import pallas as pl
from jax.experimental.pallas import tpu as pltpu
from jax.sharding import PartitionSpec as P

ITERS = 2
EPSILON = 1e-06
STEP_SCALE = 0.5
LANES = 128
CHUNK = 512
MESH = pl.DeviceIdType.MESH
F32 = jnp.float32
BF16 = jnp.bfloat16


def split(values):
    high = values.astype(BF16)
    return high, (values - high.astype(F32)).astype(BF16)


def exchange(axis, count, me, source, target, others, send, recv):
    def start(k, carry):
        peer = lax.rem(me + count - k, count)
        pltpu.make_async_remote_copy(
            src_ref=source,
            dst_ref=target(me),
            send_sem=send,
            recv_sem=recv,
            device_id={axis: peer},
            device_id_type=MESH,
        ).start()
        return carry

    lax.fori_loop(1, count, start, 0)
    return (
        lambda: pltpu.make_async_copy(others, others, recv).wait(),
        lambda: pltpu.make_async_copy(others, others, send).wait(),
    )


def segment(ids, start, width, rows, quarters):
    place = lax.broadcasted_iota(jnp.int32, (rows, LANES), 0) * LANES
    place = place + lax.broadcasted_iota(jnp.int32, (rows, LANES), 1) - start
    result = jnp.full((rows, LANES), -1, jnp.int32)
    for p, tile_id in enumerate(ids):
        for q in range(quarters):
            result = jnp.where(place == p * quarters + q, tile_id * quarters + q, result)
    return jnp.where((place >= 0) & (place < width), result, 0)


def kernel(
    n_blk,
    n_grp,
    primal,
    dual,
    objective,
    lower,
    upper,
    bound_kind,
    rhs,
    row_kind,
    q_index,
    k_rows,
    k_cols,
    q_tiles,
    k_tiles,
    x_out,
    y_out,
    w_out,
    raw,
    staged,
    kinds,
    staged_rows,
    weight_out,
    q_at,
    r_at,
    c_at,
    xs,
    ys,
    data,
    rows_data,
    ids_x,
    ids_y,
    sel_h,
    sel_t,
    sel_y,
    vals_h,
    vals_t,
    vals_y,
    sums_x,
    sums_y,
    cons_now,
    tile_sem,
    io_sem,
    blk_send,
    blk_recv,
    one_send,
    one_recv,
    grp_send,
    grp_recv,
):
    blk, grp = lax.axis_index("blk"), lax.axis_index("grp")
    nq, nk = q_tiles.shape[0], k_tiles.shape[0]
    tile = q_tiles.shape[-1]
    quarters = tile // LANES
    own_x, own_y = primal.shape[0], dual.shape[0]
    wide_h, wide_t = nq * quarters, nk * quarters
    pairs = n_blk // 2
    code_h = sel_h.shape[1] // LANES

    barrier = pltpu.get_barrier_semaphore()

    def greet(axis, count, me):
        def body(k, carry):
            pl.semaphore_signal(
                barrier, inc=1, device_id={axis: lax.rem(me + k, count)}, device_id_type=MESH
            )
            return carry

        lax.fori_loop(1, count, body, 0)

    greet("blk", n_blk, blk)
    greet("grp", n_grp, grp)

    mine_x = pl.ds(pl.multiple_of(blk * own_x, own_x), own_x)
    mine_y = pl.ds(pl.multiple_of(grp * own_y, own_y), own_y)
    fetched = []
    for source, target in (
        (dual, ys.at[mine_y]),
        (primal, xs.at[mine_x]),
        (q_index, q_at),
        (k_rows, r_at),
        (k_cols, c_at),
        (objective, data.at[0, mine_x]),
        (lower, staged.at[0]),
        (upper, staged.at[1]),
        (bound_kind, kinds),
        (rhs, rows_data.at[0, mine_y]),
        (row_kind, staged_rows),
    ):
        fetched.append(pltpu.make_async_copy(source, target, io_sem.at[len(fetched)]))
        fetched[-1].start()
    for item in fetched:
        item.wait()
    loads = []
    for t in range(nk + nq):
        source = k_tiles.at[t] if t < nk else q_tiles.at[t - nk]
        loads.append(pltpu.make_async_copy(source, raw.at[t], tile_sem.at[t]))
        loads[-1].start()

    def slot(ref, index, size):
        return ref.at[pl.ds(pl.multiple_of(index * size, size), size)]

    q_rows = [q_at[0, p] for p in range(nq)]
    q_cols = [q_at[1, p] for p in range(nq)]
    c_rows = [r_at[0, p] for p in range(nk)]
    c_cols = [c_at[0, p] for p in range(nk)]
    code_t = ids_x.shape[1] - code_h
    ids_x[blk, :code_h] = segment(q_rows, blk * wide_h, wide_h, code_h, quarters)
    ids_x[blk, code_h:] = segment(c_cols, blk * wide_t, wide_t, code_t, quarters)
    ids_y[grp] = segment(c_rows, grp * wide_t, wide_t, ids_y.shape[1], quarters)
    kind = kinds[...]
    data[1, mine_x] = jnp.where((kind == 1) | (kind == 2), staged[0], -jnp.inf)
    data[2, mine_x] = jnp.where((kind == 2) | (kind == 3), staged[1], jnp.inf)
    rows_data[1, mine_y] = jnp.where(staged_rows[...] == 1, 0.0, -jnp.inf)

    pl.semaphore_wait(barrier, n_blk + n_grp - 2)

    leaving = []
    used = {"blk": 0, "grp": 0, "two": 0}

    def share(axis, source, target, others):
        at = used[axis]
        used[axis] += 1
        count, me = (n_blk, blk) if axis == "blk" else (n_grp, grp)
        send, recv = (one_send, one_recv) if axis == "blk" else (grp_send, grp_recv)
        arrive, leave = exchange(
            axis, count, me, source, target, others, send.at[at], recv.at[at]
        )
        leaving.append(leave)
        return arrive

    y_here = share("grp", ys.at[mine_y], lambda s: slot(ys, s, own_y), ys.at[: (n_grp - 1) * own_y])

    outer, inner = lax.div(blk, 2), lax.rem(blk, 2)

    def passing(view, at, k, theirs, other):
        there = lax.rem(outer + k, pairs) * 2
        if other:
            sent, got, to = there + inner, there + 1 - inner, outer * 2 + 1 - inner
        else:
            sent, got, to = blk, there + inner, there + inner
        return pltpu.make_async_remote_copy(
            src_ref=view(sent),
            dst_ref=view(got if theirs else sent),
            send_sem=blk_send.at[at, k],
            recv_sem=blk_recv.at[at, got if theirs else sent],
            device_id={"blk": to},
            device_id_type=MESH,
        )

    def each(first, call):
        def body(k, carry):
            call(k)
            return carry

        lax.fori_loop(first, pairs, body, 0)

    def begin(view, own, other):
        passing(view, other, 0, False, True).start()
        each(1, lambda k: passing(view, own, k, False, False).start())

    def relay(view, own, other):
        def one(k):
            passing(view, own, k, True, False).wait_recv()
            passing(view, other, k, False, True).start()

        each(1, one)

    def finish(view, own, other):
        each(0, lambda k: passing(view, other, k, True, True).wait_recv())

    def depart(view, own, other):
        each(0, lambda k: passing(view, other, k, False, True).wait_send())
        each(1, lambda k: passing(view, own, k, False, False).wait_send())

    def reserve():
        used["two"] += 1
        return used["two"] - 1

    x_view = lambda s: slot(xs, s, own_x)
    x_at = (reserve(), reserve())
    begin(x_view, *x_at)
    ids_y_here = share("grp", ids_y.at[grp], lambda s: ids_y.at[s], ids_y.at[: n_grp - 1])
    def planes(ref, index, size):
        return ref.at[:, pl.ds(pl.multiple_of(index * size, size), size)]

    rows_here = share("grp", planes(rows_data, grp, own_y), lambda s: planes(rows_data, s, own_y), rows_data.at[:, : (n_grp - 1) * own_y])

    def folded(values):
        return jnp.sum(values.reshape(-1, 8, LANES), axis=0)

    def strip(vector, index, q):
        row = vector[pl.ds(index * quarters + q, 1), :]
        return jnp.broadcast_to(row, (LANES, LANES))

    def block(t, q, c):
        return raw[t, q * LANES : (q + 1) * LANES, c * LANES : (c + 1) * LANES]

    def product(vector, index, t, transposed):
        if transposed:
            total = [jnp.zeros((8, LANES), F32)] * quarters
            for q in range(quarters):
                column = strip(vector, index, q).T
                for c in range(quarters):
                    total[c] = total[c] + folded(block(t, q, c) * column)
        else:
            rows = [strip(vector, index, c) for c in range(quarters)]
            total = []
            for q in range(quarters):
                part = block(t, q, 0) * rows[0]
                for c in range(1, quarters):
                    part = part + block(t, q, c) * rows[c]
                total.append(folded(part.T))
        return [jnp.sum(part, axis=0, keepdims=True) for part in total]

    def put(ref, first, values):
        for q in range(quarters):
            ref[pl.ds(first + q, 1), :] = values[q]

    def row_block(ref, step, index, size):
        return ref.at[step, pl.ds(pl.multiple_of(index * size, 8), size)]

    def transposed(step):
        mine = row_block(vals_t, step, blk, wide_t)
        for p in range(nk):
            put(mine, p * quarters, [-part for part in product(ys, c_rows[p], p, True)])
        return share("blk", mine, lambda s: row_block(vals_t, step, s, wide_t), vals_t.at[step, : (n_blk - 1) * wide_t])

    def hessian(step):
        mine = row_block(vals_h, step, blk, wide_h)
        for p in range(nq):
            put(mine, p * quarters, product(xs, q_cols[p], nk + p, False))
        return share("blk", mine, lambda s: row_block(vals_h, step, s, wide_h), vals_h.at[step, : (n_blk - 1) * wide_h])

    def spread(axis, ref, step, value):
        me = blk if axis == "blk" else grp
        ref[step, me] = jnp.broadcast_to(value, (1, LANES))
        count = n_blk if axis == "blk" else n_grp
        return share(axis, ref.at[step, me], lambda s: ref.at[step, s], ref.at[step, : count - 1])

    def constraint(step):
        mine = row_block(vals_y, step, grp, wide_t)
        for p in range(nk):
            fresh = product(xs, c_cols[p], p, False)
            for q in range(quarters):
                part = fresh[q]
                at = pl.ds(p * quarters + q, 1)
                mine[at, :] = 2.0 * part - cons_now[at, :]
                cons_now[at, :] = part
        return share("grp", mine, lambda s: row_block(vals_y, step, s, wide_t), vals_y.at[step, : (n_grp - 1) * wide_t])

    def parts(values):
        return jnp.concatenate(split(values), axis=1)

    def gathered(*terms):
        both = sum(
            jnp.dot(selector, values, preferred_element_type=F32) for selector, values in terms
        )
        return both[:, :LANES] + both[:, LANES:]

    def scalar_sum(ref, step, count):
        total = ref[step, 0]
        for s in range(1, count):
            total = total + ref[step, s]
        return total

    def full_sum(values):
        return jnp.sum(jnp.sum(values, axis=0, keepdims=True), axis=1, keepdims=True)

    chunk_x = min(CHUNK, n_blk * own_x)
    chunk_y = min(CHUNK, n_grp * own_y)

    def selectors():
        ids_y_here()
        ids_x_here()
        codes_x, codes_y = jnp.sum(ids_x[...], axis=0), jnp.sum(ids_y[...], axis=0)
        for ref, codes, chunk in (
            (sel_h, codes_x[:code_h], chunk_x),
            (sel_t, codes_x[code_h:], chunk_x),
            (sel_y, codes_y, chunk_y),
        ):

            def body(c, carry):
                base = pl.multiple_of(c * chunk, chunk)
                at = lax.broadcasted_iota(jnp.int32, (chunk, LANES), 0) + base
                for k in range(ref.shape[1] // LANES):
                    hit = at == codes[k : k + 1, :]
                    ref[pl.ds(base, chunk), k * LANES : (k + 1) * LANES] = jnp.where(
                        hit, 1.0, 0.0
                    ).astype(BF16)
                return carry

            lax.fori_loop(0, ref.shape[0] // chunk, body, 0)

    def primal_step(step, tau):
        from_h, from_t = parts(vals_h[step]), parts(vals_t[step])

        def body(c, total):
            at = pl.ds(pl.multiple_of(c * chunk_x, chunk_x), chunk_x)
            gradient = gathered(
                (sel_h[at, : n_blk * wide_h], from_h), (sel_t[at, : n_blk * wide_t], from_t)
            )
            gradient = gradient + data[0, at]
            now = xs[at]
            new = jnp.minimum(jnp.maximum(now - tau * gradient, data[1, at]), data[2, at])
            xs[at] = new
            return total + full_sum((new - now) * (new - now))

        return lax.fori_loop(0, n_blk * own_x // chunk_x, body, jnp.zeros((1, 1), F32))

    def dual_step(step, sigma):
        values = parts(vals_y[step])

        def body(c, total):
            at = pl.ds(pl.multiple_of(c * chunk_y, chunk_y), chunk_y)
            extrap = gathered((sel_y[at, : n_grp * wide_t], values))
            now = ys[at]
            new = jnp.maximum(now + sigma * (rows_data[0, at] - extrap), rows_data[1, at])
            ys[at] = new
            return total + full_sum((new - now) * (new - now))

        return lax.fori_loop(0, n_grp * own_y // chunk_y, body, jnp.zeros((1, 1), F32))

    weight = jnp.ones((1, LANES), F32)
    for t in range(nk):
        loads[t].wait()
    y_here()
    transposed_here = transposed(0)
    ids_x_here = share("blk", ids_x.at[blk], lambda s: ids_x.at[s], ids_x.at[: n_blk - 1])
    relay(x_view, *x_at)
    views = []
    for plane in range(data.shape[0]):
        view = functools.partial(lambda plane, s: slot(data.at[plane], s, own_x), plane)
        views.append((view, reserve(), reserve()))
        begin(*views[-1])
    for t in range(nk, nk + nq):
        loads[t].wait()
    finish(x_view, *x_at)
    hessian_here = hessian(0)
    for p in range(nk):
        put(cons_now, p * quarters, product(xs, c_cols[p], p, False))
    for item in views:
        relay(*item)
    selectors()
    for item in views:
        finish(*item)
    depart(x_view, *x_at)
    for step in range(ITERS):
        hessian_here()
        transposed_here()
        if step > 0:
            dual_here()
            dual_total = scalar_sum(sums_x, step - 1, n_blk)
            weight = jnp.sqrt(
                weight * jnp.sqrt((dual_total + EPSILON) / (primal_total + EPSILON))
            )
        primal_sq = primal_step(step, STEP_SCALE / weight)
        constraint_here = constraint(step)
        if step == ITERS - 1:
            x_done = pltpu.make_async_copy(xs.at[mine_x], x_out, io_sem.at[0])
            x_done.start()
        primal_here = spread("grp", sums_y, step, primal_sq)
        if step < ITERS - 1:
            hessian_here = hessian(step + 1)
        if step == 0:
            rows_here()
            leaving.pop(0)()
        constraint_here()
        dual_sq = dual_step(step, STEP_SCALE * weight)
        dual_here = spread("blk", sums_x, step, dual_sq)
        if step < ITERS - 1:
            transposed_here = transposed(step + 1)
        primal_here()
        primal_total = scalar_sum(sums_y, step, n_grp)
    y_done = pltpu.make_async_copy(ys.at[mine_y], y_out, io_sem.at[1])
    y_done.start()
    dual_here()
    dual_total = scalar_sum(sums_x, ITERS - 1, n_blk)
    weight = jnp.sqrt(weight * jnp.sqrt((dual_total + EPSILON) / (primal_total + EPSILON)))
    weight_out[...] = weight[:, :1]
    w_done = pltpu.make_async_copy(weight_out, w_out, io_sem.at[2])
    w_done.start()
    for item in (x_done, y_done, w_done):
        item.wait()
    for item in views:
        depart(*item)
    for leave in leaving:
        leave()


def up(value, step):
    return -(-value // step) * step


def shards(
    primal,
    dual,
    objective,
    lower,
    upper,
    bound_kind,
    rhs,
    row_kind,
    q_tiles,
    q_index,
    k_tiles,
    k_rows,
    k_cols,
):
    n_blk, n_grp = lax.axis_size("blk"), lax.axis_size("grp")
    nq, nk, tile = q_tiles.shape[1], k_tiles.shape[1], q_tiles.shape[-1]
    quarters = tile // LANES
    own_x, own_y = primal.shape[0] // LANES, dual.shape[0] // LANES
    wide_h, wide_t = nq * quarters, nk * quarters
    code_h, code_t = up(n_blk * wide_h, LANES), up(n_blk * wide_t, LANES)
    code_y = up(n_grp * wide_t, LANES)
    hbm = pl.BlockSpec(memory_space=pl.ANY)

    def lanes(values):
        return values.reshape(-1, LANES)

    x, y, weight = pl.pallas_call(
        functools.partial(kernel, n_blk, n_grp),
        out_shape=(
            jax.ShapeDtypeStruct((own_x, LANES), F32),
            jax.ShapeDtypeStruct((own_y, LANES), F32),
            jax.ShapeDtypeStruct((1, 1), F32),
        ),
        in_specs=[hbm] * 13,
        out_specs=(hbm, hbm, hbm),
        scratch_shapes=[
            pltpu.VMEM((nk + nq, tile, tile), F32),
            pltpu.VMEM((2, own_x, LANES), F32),
            pltpu.VMEM((own_x, LANES), jnp.int32),
            pltpu.VMEM((own_y, LANES), jnp.int32),
            pltpu.VMEM((1, 1), F32),
            pltpu.SMEM((2, nq), jnp.int32),
            pltpu.SMEM((1, nk), jnp.int32),
            pltpu.SMEM((1, nk), jnp.int32),
            pltpu.VMEM((n_blk * own_x, LANES), F32),
            pltpu.VMEM((n_grp * own_y, LANES), F32),
            pltpu.VMEM((3, n_blk * own_x, LANES), F32),
            pltpu.VMEM((2, n_grp * own_y, LANES), F32),
            pltpu.VMEM((n_blk, (code_h + code_t) // LANES, LANES), jnp.int32),
            pltpu.VMEM((n_grp, code_y // LANES, LANES), jnp.int32),
            pltpu.VMEM((n_blk * own_x, code_h), BF16),
            pltpu.VMEM((n_blk * own_x, code_t), BF16),
            pltpu.VMEM((n_grp * own_y, code_y), BF16),
            pltpu.VMEM((ITERS, n_blk * wide_h, LANES), F32),
            pltpu.VMEM((ITERS, n_blk * wide_t, LANES), F32),
            pltpu.VMEM((ITERS, n_grp * wide_t, LANES), F32),
            pltpu.VMEM((ITERS, n_blk, 1, LANES), F32),
            pltpu.VMEM((ITERS, n_grp, 1, LANES), F32),
            pltpu.VMEM((nk * quarters, LANES), F32),
            pltpu.SemaphoreType.DMA((nk + nq,)),
            pltpu.SemaphoreType.DMA((11,)),
            pltpu.SemaphoreType.DMA((8, n_blk)),
            pltpu.SemaphoreType.DMA((8, n_blk)),
            pltpu.SemaphoreType.DMA((3 * ITERS + 1,)),
            pltpu.SemaphoreType.DMA((3 * ITERS + 1,)),
            pltpu.SemaphoreType.DMA((2 * ITERS + 3,)),
            pltpu.SemaphoreType.DMA((2 * ITERS + 3,)),
        ],
        compiler_params=pltpu.CompilerParams(
            collective_id=0, has_side_effects=True, vmem_limit_bytes=60 * 1024 * 1024
        ),
    )(
        lanes(primal),
        lanes(dual),
        lanes(objective),
        lanes(lower),
        lanes(upper),
        lanes(bound_kind),
        lanes(rhs),
        lanes(row_kind),
        q_index[0],
        k_rows,
        k_cols,
        q_tiles[0],
        k_tiles[0],
    )
    return x.reshape(-1), y.reshape(-1), weight.reshape(())


def solution(mesh):
    vector = P(("blk", "grp"))
    return jax.shard_map(
        shards,
        mesh=mesh,
        in_specs=(vector,) * 8
        + (
            P("grp", "blk", None, None),
            P("grp", None, "blk"),
            P("grp", "blk", None, None),
            P("grp", "blk"),
            P("grp", "blk"),
        ),
        out_specs=(vector, vector, P()),
        check_vma=False,
    )
```

```python
import functools

import jax
import jax.numpy as jnp
from jax import lax
from jax.experimental import pallas as pl
from jax.experimental.pallas import tpu as pltpu
from jax.sharding import PartitionSpec as P

ITERS = 2
EPSILON = 1e-06
STEP_SCALE = 0.5
LANES = 128
UNROLL = 8
FREE = 2.0**100
MESH = pl.DeviceIdType.MESH
F32 = jnp.float32
BF16 = jnp.bfloat16


def up(value, step):
    return -(-value // step) * step


def split(values, count=2):
    parts = []
    for _ in range(count):
        parts.append(values.astype(BF16))
        values = values - parts[-1].astype(F32)
    return parts


def partner(me, k, count):
    if count & (count - 1):
        return lax.rem(me + k, count)
    result = 0
    bit = 1
    while bit < count:
        mine, theirs = lax.rem(lax.div(me, bit), 2), lax.rem(lax.div(jnp.int32(k), bit), 2)
        result = result + lax.rem(mine + theirs, 2) * bit
        bit *= 2
    return result


def repeat(first, count, call):
    if count <= UNROLL:
        for k in range(first, count):
            call(k)
    else:

        def body(k, carry):
            call(k)
            return carry

        lax.fori_loop(first, count, body, 0)


def segment(ids, start, width, rows, quarters):
    place = lax.broadcasted_iota(jnp.int32, (rows, LANES), 0) * LANES
    place = place + lax.broadcasted_iota(jnp.int32, (rows, LANES), 1) - start
    result = jnp.full((rows, LANES), -1, jnp.int32)
    for p, tile_id in enumerate(ids):
        for q in range(quarters):
            result = jnp.where(place == p * quarters + q, tile_id * quarters + q, result)
    return jnp.where((place >= 0) & (place < width), result, 0)


def kernel(
    n_blk,
    n_grp,
    primal,
    dual,
    objective,
    lower,
    upper,
    bound_kind,
    rhs,
    row_kind,
    q_index,
    k_rows,
    k_cols,
    q_tiles,
    k_tiles,
    x_out,
    y_out,
    w_out,
    raw,
    kinds,
    row_kinds,
    weight_out,
    q_at,
    r_at,
    c_at,
    xs,
    ys,
    xw,
    both,
    data,
    rows_data,
    slot_out,
    slot_in,
    ids_x,
    ids_y,
    sel_h,
    sel_t,
    sel_y,
    vals_h,
    vals_t,
    vals_y,
    sums_x,
    sums_y,
    cons_now,
    tile_sem,
    io_sem,
    far_recv,
    one_send,
    one_recv,
    blk_send,
    blk_recv,
    grp_send,
    grp_recv,
):
    blk, grp = lax.axis_index("blk"), lax.axis_index("grp")
    nq, nk = q_tiles.shape[0], k_tiles.shape[0]
    quarters = q_tiles.shape[-1] // LANES
    own_x, own_y = primal.shape[0], dual.shape[0]
    wide_h, wide_t = nq * quarters, nk * quarters
    pairs = n_blk // 2
    outer, inner = lax.div(blk, 2), lax.rem(blk, 2)
    beside = outer * 2 + 1 - inner
    code_h, code_t = sel_h.shape[1] // LANES, sel_t.shape[1] // LANES
    q_first = up(wide_t, 16)
    first_k, first_q = own_x, own_x + q_first
    last = first_q + wide_h

    barrier = pltpu.get_barrier_semaphore()

    def greet(axis, count, me):
        def one(k):
            pl.semaphore_signal(
                barrier,
                inc=1,
                device_id={axis: partner(me, k, count)},
                device_id_type=MESH,
            )

        repeat(1, count, one)

    greet("blk", n_blk, blk)
    greet("grp", n_grp, grp)

    def part(index, size):
        return pl.ds(pl.multiple_of(index * size, size), size)

    fetched = []
    mine_pair = part(inner, own_x)
    for at, (source, target) in enumerate(
        (
            (dual, ys.at[part(grp, own_y)]),
            (primal, xs.at[part(blk, own_x)]),
            (q_index, q_at),
            (k_rows, r_at),
            (k_cols, c_at),
            (bound_kind, kinds),
            (rhs, rows_data.at[0, part(grp, own_y)]),
            (row_kind, row_kinds),
            (objective, both.at[0, mine_pair]),
            (lower, both.at[1, mine_pair]),
            (upper, both.at[2, mine_pair]),
        )
    ):
        fetched.append(pltpu.make_async_copy(source, target, io_sem.at[at]))
        fetched[-1].start()
    for item in fetched:
        item.wait()
    for t in range(nk):
        pltpu.make_async_copy(k_tiles.at[t], raw.at[t], tile_sem.at[0]).start()
    for t in range(nq):
        pltpu.make_async_copy(q_tiles.at[t], raw.at[nk + t], tile_sem.at[1]).start()

    q_rows = [q_at[0, p] for p in range(nq)]
    q_cols = [q_at[1, p] for p in range(nq)]
    c_rows = [r_at[0, p] for p in range(nk)]
    c_cols = [c_at[0, p] for p in range(nk)]
    ids_x[blk, :code_h] = segment(q_rows, blk * wide_h, wide_h, code_h, quarters)
    ids_x[blk, code_h : code_h + code_t] = segment(
        c_cols, blk * wide_t, wide_t, code_t, quarters
    )
    wanted = c_cols + [-1] * ((q_first - wide_t) // quarters) + q_cols
    ids_x[blk, code_h + code_t :] = segment(
        wanted, 0, q_first + wide_h, ids_x.shape[1] - code_h - code_t, quarters
    )
    ids_y[grp] = segment(c_rows, grp * wide_t, wide_t, ids_y.shape[1], quarters)
    kind = kinds[...]
    both[1, mine_pair] = jnp.where((kind == 1) | (kind == 2), both[1, mine_pair], -FREE)
    both[2, mine_pair] = jnp.where((kind == 2) | (kind == 3), both[2, mine_pair], FREE)
    rows_data[1, part(grp, own_y)] = jnp.where(row_kinds[...] == 1, 0.0, -FREE)

    pl.semaphore_wait(barrier, n_blk + n_grp - 2)

    leaving = []
    used = {"blk": 0, "grp": 0, "one": 0}

    def waiter(ref, sem):
        return lambda: pltpu.make_async_copy(ref, ref, sem).wait()

    def send(axis, peer, source, target, send_sem, recv_sem):
        pltpu.make_async_remote_copy(
            src_ref=source,
            dst_ref=target,
            send_sem=send_sem,
            recv_sem=recv_sem,
            device_id={axis: peer},
            device_id_type=MESH,
        ).start()

    def share(axis, mine, others):
        at = used[axis]
        used[axis] += 1
        count, me = (n_blk, blk) if axis == "blk" else (n_grp, grp)
        sends, recvs = (blk_send, blk_recv) if axis == "blk" else (grp_send, grp_recv)
        repeat(
            1,
            count,
            lambda k: send(
                axis, partner(me, count - k, count), mine, mine, sends.at[at], recvs.at[at]
            ),
        )
        leaving.append(waiter(others, sends.at[at]))
        return waiter(others, recvs.at[at])

    def single():
        used["one"] += 1
        return one_send.at[used["one"] - 1], one_recv.at[used["one"] - 1]

    y_here = share("grp", ys.at[part(grp, own_y)], ys.at[: (n_grp - 1) * own_y])
    ids_x_here = share("blk", ids_x.at[blk], ids_x.at[: n_blk - 1])

    far_send = single()[0]
    near_send, near_recv = single()

    def x_slot(s):
        return xs.at[part(s, own_x)]

    def x_far(k):
        send(
            "blk",
            partner(outer, pairs - k, pairs) * 2 + inner,
            x_slot(blk),
            x_slot(blk),
            far_send,
            far_recv.at[outer],
        )

    def x_relay(k):
        there = partner(outer, k, pairs)
        source = x_slot(there * 2 + inner)
        waiter(source, far_recv.at[there])()
        send("blk", beside, source, source, near_send, near_recv)

    repeat(1, pairs, x_far)
    send("blk", beside, x_slot(blk), x_slot(blk), near_send, near_recv)
    x_here = waiter(xs.at[: pairs * own_x], near_recv)
    leaving.append(waiter(xs.at[: (pairs - 1) * own_x], far_send))
    leaving.append(waiter(xs.at[: pairs * own_x], near_send))

    planes_send, planes_recv = single()
    planes = both.at[:, mine_pair]
    send("blk", beside, planes, planes, planes_send, planes_recv)
    planes_here = waiter(planes, planes_recv)
    leaving.append(waiter(planes, planes_send))

    ids_y_here = share("grp", ids_y.at[grp], ids_y.at[: n_grp - 1])
    rows_here = share(
        "grp", rows_data.at[:, part(grp, own_y)], rows_data.at[:, : (n_grp - 1) * own_y]
    )

    xw[:own_x] = xs[part(blk, own_x)]
    data[:, :own_x] = both[:, mine_pair]
    xw[first_k + wide_t : first_q] = jnp.zeros((q_first - wide_t, LANES), F32)
    data[:, first_k + wide_t : first_q] = jnp.zeros((3, q_first - wide_t, LANES), F32)

    def folded(values):
        return jnp.sum(values.reshape(-1, 8, LANES), axis=0)

    def strip(vector, first, q):
        return jnp.broadcast_to(vector[pl.ds(first + q, 1), :], (LANES, LANES))

    def block(t, q, c):
        return raw[t, q * LANES : (q + 1) * LANES, c * LANES : (c + 1) * LANES]

    def product(vector, first, t, transposed):
        if transposed:
            total = [jnp.zeros((8, LANES), F32)] * quarters
            for q in range(quarters):
                column = strip(vector, first, q).T
                for c in range(quarters):
                    total[c] = total[c] + folded(block(t, q, c) * column)
        else:
            rows = [strip(vector, first, c) for c in range(quarters)]
            total = []
            for q in range(quarters):
                piece = block(t, q, 0) * rows[0]
                for c in range(1, quarters):
                    piece = piece + block(t, q, c) * rows[c]
                total.append(folded(piece.T))
        return [jnp.sum(piece, axis=0, keepdims=True) for piece in total]

    def row_block(ref, step, index, size):
        return ref.at[step, pl.ds(pl.multiple_of(index * size, 8), size)]

    def transposed(step):
        mine = row_block(vals_t, step, blk, wide_t)
        for p in range(nk):
            for q, piece in enumerate(product(ys, c_rows[p] * quarters, p, True)):
                mine[pl.ds(p * quarters + q, 1), :] = -piece
        return share("blk", mine, vals_t.at[step, : (n_blk - 1) * wide_t])

    def hessian(step):
        mine = row_block(vals_h, step, blk, wide_h)
        for p in range(nq):
            for q, piece in enumerate(product(xw, first_q + p * quarters, nk + p, False)):
                mine[pl.ds(p * quarters + q, 1), :] = piece
        return share("blk", mine, vals_h.at[step, : (n_blk - 1) * wide_h])

    def constraint_now(call):
        for p in range(nk):
            for q, piece in enumerate(product(xw, first_k + p * quarters, p, False)):
                call(pl.ds(p * quarters + q, 1), piece)

    def constraint(step):
        mine = row_block(vals_y, step, grp, wide_t)

        def put(at, piece):
            mine[at, :] = 2.0 * piece - cons_now[at, :]
            if step < ITERS - 1:
                cons_now[at, :] = piece

        constraint_now(put)
        return share("grp", mine, vals_y.at[step, : (n_grp - 1) * wide_t])

    def spread(axis, ref, step, value):
        me, count = (blk, n_blk) if axis == "blk" else (grp, n_grp)
        ref[step, me] = jnp.broadcast_to(value, (1, LANES))
        return share(axis, ref.at[step, me], ref.at[step, : count - 1])

    def parts(values):
        return jnp.concatenate(split(values), axis=1)

    def gathered(*terms):
        total = sum(
            jnp.dot(selector, values, preferred_element_type=F32) for selector, values in terms
        )
        return total[:, :LANES] + total[:, LANES:]

    def scalar_sum(ref, step, count):
        total = ref[step, 0]
        for s in range(1, count):
            total = total + ref[step, s]
        return total

    def full_sum(values):
        return jnp.sum(jnp.sum(values, axis=0, keepdims=True), axis=1, keepdims=True)

    def selector(ref, place, codes):
        for k in range(ref.shape[1] // LANES):
            ref[:, k * LANES : (k + 1) * LANES] = jnp.where(
                place == codes[k : k + 1, :], 1.0, 0.0
            ).astype(BF16)

    def selectors():
        ids_y_here()
        codes = jnp.sum(ids_x[:, : code_h + code_t], axis=0)
        line = lax.broadcasted_iota(jnp.int32, (last, LANES), 0)
        place = jnp.where(line < own_x, line + blk * own_x, -1)
        for ids, first in ((c_cols, first_k), (q_cols, first_q)):
            for p, tile_id in enumerate(ids):
                begin = first + p * quarters
                inside = (line >= begin) & (line < begin + quarters)
                place = jnp.where(inside, line - begin + tile_id * quarters, place)
        selector(sel_h, place, codes[:code_h])
        selector(sel_t, place, codes[code_h:])
        line = lax.broadcasted_iota(jnp.int32, (sel_y.shape[0], LANES), 0)
        selector(sel_y, line, jnp.sum(ids_y[...], axis=0))

    def picked():
        values = jnp.concatenate(
            [piece for plane in range(3) for piece in split(both[plane], 3)], axis=1
        )
        line = lax.broadcasted_iota(jnp.int32, (2 * own_x, LANES), 0) + outer * (2 * own_x)

        def one(k):
            there = partner(outer, k, pairs)
            codes = ids_x[there * 2 + inner, code_h + code_t :]
            hits = jnp.where(line == codes, 1.0, 0.0).T[: slot_out.shape[2]].astype(BF16)
            taken = jnp.dot(hits, values, preferred_element_type=F32)
            for plane in range(3):
                pieces = [
                    taken[:, (plane * 3 + i) * LANES : (plane * 3 + i + 1) * LANES]
                    for i in range(3)
                ]
                slot_out[there, plane] = pieces[0] + (pieces[1] + pieces[2])

        repeat(0, pairs, one)

    def hand_out(first, width):
        send_sem, recv_sem = single()

        def one(k):
            there = partner(outer, pairs - k, pairs)
            send(
                "blk",
                there * 2 + inner,
                slot_out.at[there, :, first : first + width],
                slot_in.at[outer, :, first : first + width],
                send_sem,
                recv_sem,
            )

        repeat(1, pairs, one)
        whole = slot_in.at[: pairs - 1, :, first : first + width]
        leaving.append(waiter(whole, send_sem))
        here = waiter(whole, recv_sem)

        def take():
            here()
            total = slot_out[outer, :, first : first + width]
            if pairs <= UNROLL:
                for k in range(1, pairs):
                    total = total + slot_in[partner(outer, k, pairs), :, first : first + width]
            else:
                total = lax.fori_loop(
                    1,
                    pairs,
                    lambda k, so_far: so_far
                    + slot_in[partner(outer, k, pairs), :, first : first + width],
                    total,
                )
            data[:, own_x + first : own_x + first + width] = total

        return take

    def primal_step(step, tau, first, end):
        at = slice(first, end)
        gradient = gathered(
            (sel_h[at, : n_blk * wide_h], parts(vals_h[step])),
            (sel_t[at, : n_blk * wide_t], parts(vals_t[step])),
        )
        gradient = gradient + data[0, at]
        now = xw[at]
        new = jnp.minimum(jnp.maximum(now - tau * gradient, data[1, at]), data[2, at])
        xw[at] = new
        return (new - now) * (new - now)

    def dual_step(step, sigma):
        extrap = gathered((sel_y[:, : n_grp * wide_t], parts(vals_y[step])))
        now = ys[...]
        new = jnp.maximum(now + sigma * (rows_data[0] - extrap), rows_data[1])
        ys[...] = new
        return full_sum((new - now) * (new - now))

    weight = jnp.ones((1, 1), F32)
    waiter(raw.at[:nk], tile_sem.at[0])()
    y_here()
    transposed_here = transposed(0)
    repeat(1, pairs - 1, x_relay)
    planes_here()
    ids_x_here()
    picked()
    take_k = hand_out(0, wide_t)
    x_relay(pairs - 1)
    selectors()
    waiter(raw.at[nk:], tile_sem.at[1])()
    x_here()
    for ids, first in ((q_cols, first_q), (c_cols, first_k)):
        for p, tile_id in enumerate(ids):
            begin = first + p * quarters
            xw[begin : begin + quarters] = xs[pl.ds(tile_id * quarters, quarters)]
    hessian_here = hessian(0)
    take_q = hand_out(q_first, wide_h)

    def keep(at, piece):
        cons_now[at, :] = piece

    constraint_now(keep)
    take_k()
    for step in range(ITERS):
        hessian_here()
        transposed_here()
        if step > 0:
            dual_here()
            total = scalar_sum(sums_x, step - 1, n_blk)
            ratio = (total[:, :1] + EPSILON) / (total[:, LANES // 2 : LANES // 2 + 1] + EPSILON)
            weight = jnp.sqrt(weight * jnp.sqrt(ratio))
        tau = STEP_SCALE / weight
        moved = full_sum(primal_step(step, tau, 0, first_q)[:own_x])
        constraint_here = constraint(step)
        primal_here = spread("grp", sums_y, step, moved)
        if step < ITERS - 1:
            take_q()
            primal_step(step, tau, first_q, last)
            hessian_here = hessian(step + 1)
        else:
            x_done = pltpu.make_async_copy(xw.at[:own_x], x_out, io_sem.at[0])
            x_done.start()
        if step == 0:
            rows_here()
            leaving.pop(0)()
        constraint_here()
        gone = dual_step(step, STEP_SCALE * weight)
        primal_here()
        lane = lax.broadcasted_iota(jnp.int32, (1, LANES), 1)
        moved = jnp.where(lane < LANES // 2, gone, scalar_sum(sums_y, step, n_grp))
        dual_here = spread("blk", sums_x, step, moved)
        if step < ITERS - 1:
            transposed_here = transposed(step + 1)
    y_done = pltpu.make_async_copy(ys.at[part(grp, own_y)], y_out, io_sem.at[1])
    y_done.start()
    dual_here()
    total = scalar_sum(sums_x, ITERS - 1, n_blk)
    ratio = (total[:, :1] + EPSILON) / (total[:, LANES // 2 : LANES // 2 + 1] + EPSILON)
    weight_out[...] = jnp.sqrt(weight * jnp.sqrt(ratio))
    w_done = pltpu.make_async_copy(weight_out, w_out, io_sem.at[2])
    w_done.start()
    for leave in leaving:
        leave()
    for item in (x_done, y_done, w_done):
        item.wait()


def shards(
    primal,
    dual,
    objective,
    lower,
    upper,
    bound_kind,
    rhs,
    row_kind,
    q_tiles,
    q_index,
    k_tiles,
    k_rows,
    k_cols,
):
    n_blk, n_grp = lax.axis_size("blk"), lax.axis_size("grp")
    nq, nk, tile = q_tiles.shape[1], k_tiles.shape[1], q_tiles.shape[-1]
    quarters = tile // LANES
    own_x, own_y = primal.shape[0] // LANES, dual.shape[0] // LANES
    wide_h, wide_t = nq * quarters, nk * quarters
    code_h, code_t = up(n_blk * wide_h, LANES), up(n_blk * wide_t, LANES)
    code_y = up(n_grp * wide_t, LANES)
    slots = up(wide_t, 16) + wide_h
    pairs = n_blk // 2
    hbm = pl.BlockSpec(memory_space=pl.ANY)

    def lanes(values):
        return values.reshape(-1, LANES)

    x, y, weight = pl.pallas_call(
        functools.partial(kernel, n_blk, n_grp),
        out_shape=(
            jax.ShapeDtypeStruct((own_x, LANES), F32),
            jax.ShapeDtypeStruct((own_y, LANES), F32),
            jax.ShapeDtypeStruct((1, 1), F32),
        ),
        in_specs=[hbm] * 13,
        out_specs=(hbm, hbm, hbm),
        scratch_shapes=[
            pltpu.VMEM((nk + nq, tile, tile), F32),
            pltpu.VMEM((own_x, LANES), jnp.int32),
            pltpu.VMEM((own_y, LANES), jnp.int32),
            pltpu.VMEM((1, 1), F32),
            pltpu.SMEM((2, nq), jnp.int32),
            pltpu.SMEM((1, nk), jnp.int32),
            pltpu.SMEM((1, nk), jnp.int32),
            pltpu.VMEM((n_blk * own_x, LANES), F32),
            pltpu.VMEM((n_grp * own_y, LANES), F32),
            pltpu.VMEM((own_x + slots, LANES), F32),
            pltpu.VMEM((3, 2 * own_x, LANES), F32),
            pltpu.VMEM((3, own_x + slots, LANES), F32),
            pltpu.VMEM((2, n_grp * own_y, LANES), F32),
            pltpu.VMEM((pairs, 3, slots, LANES), F32),
            pltpu.VMEM((pairs, 3, slots, LANES), F32),
            pltpu.VMEM((n_blk, (code_h + code_t) // LANES + 1, LANES), jnp.int32),
            pltpu.VMEM((n_grp, code_y // LANES, LANES), jnp.int32),
            pltpu.VMEM((own_x + slots, code_h), BF16),
            pltpu.VMEM((own_x + slots, code_t), BF16),
            pltpu.VMEM((n_grp * own_y, code_y), BF16),
            pltpu.VMEM((ITERS, n_blk * wide_h, LANES), F32),
            pltpu.VMEM((ITERS, n_blk * wide_t, LANES), F32),
            pltpu.VMEM((ITERS, n_grp * wide_t, LANES), F32),
            pltpu.VMEM((ITERS, n_blk, 1, LANES), F32),
            pltpu.VMEM((ITERS, n_grp, 1, LANES), F32),
            pltpu.VMEM((wide_t, LANES), F32),
            pltpu.SemaphoreType.DMA((2,)),
            pltpu.SemaphoreType.DMA((11,)),
            pltpu.SemaphoreType.DMA((pairs,)),
            pltpu.SemaphoreType.DMA((5,)),
            pltpu.SemaphoreType.DMA((5,)),
            pltpu.SemaphoreType.DMA((3 * ITERS + 1,)),
            pltpu.SemaphoreType.DMA((3 * ITERS + 1,)),
            pltpu.SemaphoreType.DMA((2 * ITERS + 3,)),
            pltpu.SemaphoreType.DMA((2 * ITERS + 3,)),
        ],
        compiler_params=pltpu.CompilerParams(
            collective_id=0, has_side_effects=True, vmem_limit_bytes=60 * 1024 * 1024
        ),
    )(
        lanes(primal),
        lanes(dual),
        lanes(objective),
        lanes(lower),
        lanes(upper),
        lanes(bound_kind),
        lanes(rhs),
        lanes(row_kind),
        q_index[0],
        k_rows,
        k_cols,
        q_tiles[0],
        k_tiles[0],
    )
    return x.reshape(-1), y.reshape(-1), weight.reshape(())


def solution(mesh):
    vector = P(("blk", "grp"))
    return jax.shard_map(
        shards,
        mesh=mesh,
        in_specs=(vector,) * 8
        + (
            P("grp", "blk", None, None),
            P("grp", None, "blk"),
            P("grp", "blk", None, None),
            P("grp", "blk"),
            P("grp", "blk"),
        ),
        out_specs=(vector, vector, P()),
        check_vma=False,
    )
```

```python
import functools

import jax
import jax.numpy as jnp
from jax import lax
from jax.experimental import pallas as pl
from jax.experimental.pallas import tpu as pltpu
from jax.sharding import PartitionSpec as P

ITERS = 2
EPSILON = 1e-06
STEP_SCALE = 0.5
LANES = 128
UNROLL = 8
FREE = 2.0**100
MESH = pl.DeviceIdType.MESH
F32 = jnp.float32
BF16 = jnp.bfloat16


def up(value, step):
    return -(-value // step) * step


def split(values, count=2):
    parts = []
    for _ in range(count):
        parts.append(values.astype(BF16))
        values = values - parts[-1].astype(F32)
    return parts


def partner(me, k, count):
    if count & (count - 1):
        return lax.rem(me + k, count)
    result = 0
    bit = 1
    while bit < count:
        mine, theirs = lax.rem(lax.div(me, bit), 2), lax.rem(lax.div(jnp.int32(k), bit), 2)
        result = result + lax.rem(mine + theirs, 2) * bit
        bit *= 2
    return result


def repeat(first, count, call):
    if count <= UNROLL:
        for k in range(first, count):
            call(k)
    else:

        def body(k, carry):
            call(k)
            return carry

        lax.fori_loop(first, count, body, 0)


def segment(ids, start, width, rows, quarters):
    place = lax.broadcasted_iota(jnp.int32, (rows, LANES), 0) * LANES
    place = place + lax.broadcasted_iota(jnp.int32, (rows, LANES), 1) - start
    result = jnp.full((rows, LANES), -1, jnp.int32)
    for p, tile_id in enumerate(ids):
        for q in range(quarters):
            result = jnp.where(place == p * quarters + q, tile_id * quarters + q, result)
    return jnp.where((place >= 0) & (place < width), result, 0)


def kernel(
    n_blk,
    n_grp,
    primal,
    dual,
    objective,
    lower,
    upper,
    bound_kind,
    rhs,
    row_kind,
    q_index,
    k_rows,
    k_cols,
    q_tiles,
    k_tiles,
    x_out,
    y_out,
    w_out,
    raw,
    kinds,
    row_kinds,
    q_at,
    r_at,
    c_at,
    xs,
    ys,
    xw,
    both,
    data,
    rows_data,
    slot_out,
    slot_in,
    ids_x,
    ids_y,
    sel_h,
    sel_t,
    sel_y,
    vals_h,
    vals_t,
    vals_y,
    sums_x,
    sums_y,
    cons_now,
    tile_sem,
    io_sem,
    far_recv,
    one_send,
    one_recv,
    blk_send,
    blk_recv,
    grp_send,
    grp_recv,
):
    blk, grp = lax.axis_index("blk"), lax.axis_index("grp")
    nq, nk = q_tiles.shape[0], k_tiles.shape[0]
    quarters = q_tiles.shape[-1] // LANES
    own_x, own_y = primal.shape[0], dual.shape[0]
    half_x = own_x // 2
    wide_h, wide_t = nq * quarters, nk * quarters
    pairs = n_blk // 2
    outer, inner = lax.div(blk, 2), lax.rem(blk, 2)
    beside = outer * 2 + 1 - inner
    code_h, code_t = sel_h.shape[1] // LANES, sel_t.shape[1] // LANES
    q_first = up(wide_t, 16)
    first_k, first_q = own_x, own_x + q_first
    last = first_q + wide_h

    barrier = pltpu.get_barrier_semaphore()

    def greet(axis, count, me):
        def one(k):
            pl.semaphore_signal(
                barrier,
                inc=1,
                device_id={axis: partner(me, k, count)},
                device_id_type=MESH,
            )

        repeat(1, count, one)

    greet("blk", n_blk, blk)
    greet("grp", n_grp, grp)

    def part(index, size):
        return pl.ds(pl.multiple_of(index * size, size), size)

    fetched = []
    mine_pair = part(inner, own_x)
    for at, (source, target) in enumerate(
        (
            (dual, ys.at[part(grp, own_y)]),
            (primal.at[:half_x], xs.at[0, blk]),
            (primal.at[half_x:], xs.at[1, blk]),
            (q_index, q_at),
            (k_rows, r_at),
            (k_cols, c_at),
            (bound_kind, kinds),
            (rhs, rows_data.at[0, part(grp, own_y)]),
            (row_kind, row_kinds),
            (objective, both.at[0, mine_pair]),
            (lower, both.at[1, mine_pair]),
            (upper, both.at[2, mine_pair]),
        )
    ):
        fetched.append(pltpu.make_async_copy(source, target, io_sem.at[at]))
        fetched[-1].start()
    for item in fetched:
        item.wait()
    for t in range(nk):
        pltpu.make_async_copy(k_tiles.at[t], raw.at[t], tile_sem.at[0]).start()
    for t in range(nq):
        pltpu.make_async_copy(q_tiles.at[t], raw.at[nk + t], tile_sem.at[1]).start()

    q_rows = [q_at[0, p] for p in range(nq)]
    q_cols = [q_at[1, p] for p in range(nq)]
    c_rows = [r_at[0, p] for p in range(nk)]
    c_cols = [c_at[0, p] for p in range(nk)]
    ids_x[blk, :code_h] = segment(q_rows, blk * wide_h, wide_h, code_h, quarters)
    ids_x[blk, code_h : code_h + code_t] = segment(
        c_cols, blk * wide_t, wide_t, code_t, quarters
    )
    wanted = c_cols + [-1] * ((q_first - wide_t) // quarters) + q_cols
    ids_x[blk, code_h + code_t :] = segment(
        wanted, 0, q_first + wide_h, ids_x.shape[1] - code_h - code_t, quarters
    )
    ids_y[grp] = segment(c_rows, grp * wide_t, wide_t, ids_y.shape[1], quarters)
    kind = kinds[...]
    both[1, mine_pair] = jnp.where((kind == 1) | (kind == 2), both[1, mine_pair], -FREE)
    both[2, mine_pair] = jnp.where((kind == 2) | (kind == 3), both[2, mine_pair], FREE)
    rows_data[1, part(grp, own_y)] = jnp.where(row_kinds[...] == 1, 0.0, -FREE)

    pl.semaphore_wait(barrier, n_blk + n_grp - 2)

    leaving = []
    used = {"blk": 0, "grp": 0, "one": 0}

    def waiter(ref, sem):
        return lambda: pltpu.make_async_copy(ref, ref, sem).wait()

    def send(axis, peer, source, target, send_sem, recv_sem):
        pltpu.make_async_remote_copy(
            src_ref=source,
            dst_ref=target,
            send_sem=send_sem,
            recv_sem=recv_sem,
            device_id={axis: peer},
            device_id_type=MESH,
        ).start()

    def channel(axis, others):
        at = used[axis]
        used[axis] += 1
        count, me = (n_blk, blk) if axis == "blk" else (n_grp, grp)
        sends, recvs = (blk_send, blk_recv) if axis == "blk" else (grp_send, grp_recv)
        leaving.append(waiter(others, sends.at[at]))

        def post(mine):
            repeat(
                1,
                count,
                lambda k: send(
                    axis, partner(me, count - k, count), mine, mine, sends.at[at], recvs.at[at]
                ),
            )

        return post, waiter(others, recvs.at[at])

    def share(axis, mine, others):
        post, here = channel(axis, others)
        post(mine)
        return here

    def single():
        used["one"] += 1
        return one_send.at[used["one"] - 1], one_recv.at[used["one"] - 1]

    y_here = share("grp", ys.at[part(grp, own_y)], ys.at[: (n_grp - 1) * own_y])
    ids_x_here = share("blk", ids_x.at[blk], ids_x.at[: n_blk - 1])

    def column(ref, recvs):
        far_send = single()[0]
        near_send, near_recv = single()
        leaving.append(waiter(ref.at[: pairs - 1], far_send))
        leaving.append(waiter(ref.at[:pairs], near_send))

        def far():
            def one(k):
                there = partner(outer, pairs - k, pairs) * 2 + inner
                send("blk", there, ref.at[blk], ref.at[blk], far_send, recvs.at[outer])

            repeat(1, pairs, one)

        def near():
            send("blk", beside, ref.at[blk], ref.at[blk], near_send, near_recv)

        def relay(k):
            there = partner(outer, k, pairs)
            source = ref.at[there * 2 + inner]
            waiter(source, recvs.at[there])()
            send("blk", beside, source, source, near_send, near_recv)

        return far, near, relay, waiter(ref.at[:pairs], near_recv)

    lots = [column(xs.at[half], far_recv.at[half]) for half in range(xs.shape[0])]
    for x_far, x_near, _, _ in lots:
        x_far()
        x_near()

    planes_send, planes_recv = single()
    planes = both.at[:, mine_pair]
    send("blk", beside, planes, planes, planes_send, planes_recv)
    planes_here = waiter(planes, planes_recv)
    leaving.append(waiter(planes, planes_send))

    ids_y_here = share("grp", ids_y.at[grp], ids_y.at[: n_grp - 1])
    rows_here = share(
        "grp", rows_data.at[:, part(grp, own_y)], rows_data.at[:, : (n_grp - 1) * own_y]
    )

    xw[:half_x] = xs[0, blk]
    xw[half_x:own_x] = xs[1, blk]
    data[:, :own_x] = both[:, mine_pair]
    xw[first_k + wide_t : first_q] = jnp.zeros((q_first - wide_t, LANES), F32)
    data[:, first_k + wide_t : first_q] = jnp.zeros((3, q_first - wide_t, LANES), F32)

    def folded(values):
        return jnp.sum(values.reshape(-1, 8, LANES), axis=0)

    def strip(vector, first, q):
        return jnp.broadcast_to(vector[pl.ds(first + q, 1), :], (LANES, LANES))

    def block(t, q, c):
        return raw[t, q * LANES : (q + 1) * LANES, c * LANES : (c + 1) * LANES]

    def product(vector, first, t, transposed):
        if transposed:
            total = [jnp.zeros((8, LANES), F32)] * quarters
            for q in range(quarters):
                column = strip(vector, first, q).T
                for c in range(quarters):
                    total[c] = total[c] + folded(block(t, q, c) * column)
        else:
            rows = [strip(vector, first, c) for c in range(quarters)]
            total = []
            for q in range(quarters):
                piece = block(t, q, 0) * rows[0]
                for c in range(1, quarters):
                    piece = piece + block(t, q, c) * rows[c]
                total.append(folded(piece.T))
        return [jnp.sum(piece, axis=0, keepdims=True) for piece in total]

    def computed(count, mine, post, one):
        for p in range(count):
            one(p)
        post(mine)

    def transpose_one(step, p):
        for q, piece in enumerate(product(ys, c_rows[p] * quarters, p, True)):
            vals_t[step, blk, pl.ds(p * quarters + q, 1), :] = -piece

    def transposed(step):
        post, here = channel("blk", vals_t.at[step, : n_blk - 1])
        computed(nk, vals_t.at[step, blk], post, lambda p: transpose_one(step, p))
        return here

    def hessian(step):
        post, here = channel("blk", vals_h.at[step, : n_blk - 1])

        def one(p):
            for q, piece in enumerate(product(xw, first_q + p * quarters, nk + p, False)):
                vals_h[step, blk, pl.ds(p * quarters + q, 1), :] = piece

        computed(nq, vals_h.at[step, blk], post, one)
        return here

    def constraint_one(p, call):
        for q, piece in enumerate(product(xw, first_k + p * quarters, p, False)):
            call(pl.ds(p * quarters + q, 1), piece)

    def constraint(step):
        post, here = channel("grp", vals_y.at[step, : n_grp - 1])

        def put(at, piece):
            vals_y[step, grp, at, :] = 2.0 * piece - cons_now[at, :]
            if step < ITERS - 1:
                cons_now[at, :] = piece

        computed(nk, vals_y.at[step, grp], post, lambda p: constraint_one(p, put))
        return here

    def spread(axis, ref, step, value):
        me, count = (blk, n_blk) if axis == "blk" else (grp, n_grp)
        ref[step, me] = jnp.broadcast_to(value, (1, LANES))
        return share(axis, ref.at[step, me], ref.at[step, : count - 1])

    def parts(values):
        return jnp.concatenate(split(values), axis=1)

    def gathered(*terms):
        total = sum(
            jnp.dot(selector, values, preferred_element_type=F32) for selector, values in terms
        )
        return total[:, :LANES] + total[:, LANES:]

    def scalar_sum(ref, step, count):
        total = ref[step, 0]
        for s in range(1, count):
            total = total + ref[step, s]
        return total

    def full_sum(values):
        return jnp.sum(jnp.sum(values, axis=0, keepdims=True), axis=1, keepdims=True)

    def selector(ref, place, codes):
        for k in range(ref.shape[1] // LANES):
            ref[:, k * LANES : (k + 1) * LANES] = jnp.where(
                place == codes[k : k + 1, :], 1.0, 0.0
            ).astype(BF16)

    def selectors():
        ids_y_here()
        codes = jnp.sum(ids_x[:, : code_h + code_t], axis=0)
        line = lax.broadcasted_iota(jnp.int32, (last, LANES), 0)
        place = jnp.where(line < own_x, line + blk * own_x, -1)
        for ids, first in ((c_cols, first_k), (q_cols, first_q)):
            for p, tile_id in enumerate(ids):
                begin = first + p * quarters
                inside = (line >= begin) & (line < begin + quarters)
                place = jnp.where(inside, line - begin + tile_id * quarters, place)
        selector(sel_h, place, codes[:code_h])
        selector(sel_t, place, codes[code_h:])
        line = lax.broadcasted_iota(jnp.int32, (sel_y.shape[0], LANES), 0)
        selector(sel_y, line, jnp.sum(ids_y[...], axis=0))

    def picked():
        values = jnp.concatenate(
            [piece for plane in range(3) for piece in split(both[plane], 3)], axis=1
        )
        line = lax.broadcasted_iota(jnp.int32, (2 * own_x, LANES), 0) + outer * (2 * own_x)

        def one(k):
            there = partner(outer, k, pairs)
            codes = ids_x[there * 2 + inner, code_h + code_t :]
            hits = jnp.where(line == codes, 1.0, 0.0).T[: slot_out.shape[2]].astype(BF16)
            taken = jnp.dot(hits, values, preferred_element_type=F32)
            for plane in range(3):
                pieces = [
                    taken[:, (plane * 3 + i) * LANES : (plane * 3 + i + 1) * LANES]
                    for i in range(3)
                ]
                slot_out[there, plane] = pieces[0] + (pieces[1] + pieces[2])

        repeat(0, pairs, one)

    def hand_out(first, width):
        send_sem, recv_sem = single()

        def one(k):
            there = partner(outer, pairs - k, pairs)
            send(
                "blk",
                there * 2 + inner,
                slot_out.at[there, :, first : first + width],
                slot_in.at[outer, :, first : first + width],
                send_sem,
                recv_sem,
            )

        repeat(1, pairs, one)
        whole = slot_in.at[: pairs - 1, :, first : first + width]
        leaving.append(waiter(whole, send_sem))
        here = waiter(whole, recv_sem)

        def take():
            here()
            total = slot_out[outer, :, first : first + width]
            if pairs <= UNROLL:
                for k in range(1, pairs):
                    total = total + slot_in[partner(outer, k, pairs), :, first : first + width]
            else:
                total = lax.fori_loop(
                    1,
                    pairs,
                    lambda k, so_far: so_far
                    + slot_in[partner(outer, k, pairs), :, first : first + width],
                    total,
                )
            data[:, own_x + first : own_x + first + width] = total

        return take

    def primal_step(step, tau, first, end):
        at = slice(first, end)
        gradient = gathered(
            (sel_h[at, : n_blk * wide_h], parts(vals_h[step].reshape(n_blk * wide_h, LANES))),
            (sel_t[at, : n_blk * wide_t], parts(vals_t[step].reshape(n_blk * wide_t, LANES))),
        )
        gradient = gradient + data[0, at]
        now = xw[at]
        new = jnp.minimum(jnp.maximum(now - tau * gradient, data[1, at]), data[2, at])
        xw[at] = new
        return (new - now) * (new - now)

    def dual_step(step, sigma):
        extrap = gathered((sel_y[:, : n_grp * wide_t], parts(vals_y[step].reshape(n_grp * wide_t, LANES))))
        now = ys[...]
        new = jnp.maximum(now + sigma * (rows_data[0] - extrap), rows_data[1])
        ys[...] = new
        return full_sum((new - now) * (new - now))

    weight = jnp.ones((1, 1), F32)
    repeat(1, pairs, lots[0][2])
    waiter(raw.at[:nk], tile_sem.at[0])()
    y_here()
    for p in range(nk):
        transpose_one(0, p)
    t_far, t_near, t_relay, transposed_here = column(vals_t.at[0], far_recv.at[2])
    t_far()
    repeat(1, pairs, lots[1][2])
    t_near()
    planes_here()
    ids_x_here()
    picked()
    take_k = hand_out(0, wide_t)
    selectors()
    waiter(raw.at[nk:], tile_sem.at[1])()
    lots[0][3]()
    lots[1][3]()
    for ids, first in ((q_cols, first_q), (c_cols, first_k)):
        for p, tile_id in enumerate(ids):
            begin = first + p * quarters
            piece = lax.div(tile_id * quarters, half_x)
            at = lax.rem(tile_id * quarters, half_x)
            xw[begin : begin + quarters] = xs[
                lax.rem(piece, 2), lax.div(piece, 2), pl.ds(at, quarters)
            ]
    hessian_here = hessian(0)
    take_q = hand_out(q_first, wide_h)
    repeat(1, pairs, t_relay)

    def keep(at, piece):
        cons_now[at, :] = piece

    for p in range(nk):
        constraint_one(p, keep)
    take_k()
    for step in range(ITERS):
        hessian_here()
        transposed_here()
        if step > 0:
            dual_here()
            total = scalar_sum(sums_x, step - 1, n_blk)
            ratio = (total[:, :1] + EPSILON) / (total[:, LANES // 2 : LANES // 2 + 1] + EPSILON)
            weight = jnp.sqrt(weight * jnp.sqrt(ratio))
        tau = STEP_SCALE / weight
        moved = full_sum(primal_step(step, tau, 0, first_q)[:own_x])
        constraint_here = constraint(step)
        primal_here = spread("grp", sums_y, step, moved)
        if step < ITERS - 1:
            take_q()
            primal_step(step, tau, first_q, last)
            hessian_here = hessian(step + 1)
        else:
            x_out[...] = xw[:own_x]
        if step == 0:
            rows_here()
            leaving.pop(0)()
        constraint_here()
        gone = dual_step(step, STEP_SCALE * weight)
        primal_here()
        lane = lax.broadcasted_iota(jnp.int32, (1, LANES), 1)
        moved = jnp.where(lane < LANES // 2, gone, scalar_sum(sums_y, step, n_grp))
        dual_here = spread("blk", sums_x, step, moved)
        if step < ITERS - 1:
            transposed_here = transposed(step + 1)
    y_out[...] = ys[part(grp, own_y)]
    dual_here()
    total = scalar_sum(sums_x, ITERS - 1, n_blk)
    ratio = (total[:, :1] + EPSILON) / (total[:, LANES // 2 : LANES // 2 + 1] + EPSILON)
    w_out[...] = jnp.broadcast_to(jnp.sqrt(weight * jnp.sqrt(ratio)), w_out.shape)
    for leave in leaving:
        leave()


def settle(x, y, weight, x_out, y_out, w_out, single, sems):
    single[...] = weight[:1, :1]
    copies = [
        pltpu.make_async_copy(source, target, sems.at[at])
        for at, (source, target) in enumerate(((x, x_out), (y, y_out), (single, w_out)))
    ]
    for copy in copies:
        copy.start()
    for copy in copies:
        copy.wait()


def shards(
    primal,
    dual,
    objective,
    lower,
    upper,
    bound_kind,
    rhs,
    row_kind,
    q_tiles,
    q_index,
    k_tiles,
    k_rows,
    k_cols,
):
    n_blk, n_grp = lax.axis_size("blk"), lax.axis_size("grp")
    nq, nk, tile = q_tiles.shape[1], k_tiles.shape[1], q_tiles.shape[-1]
    quarters = tile // LANES
    own_x, own_y = primal.shape[0] // LANES, dual.shape[0] // LANES
    wide_h, wide_t = nq * quarters, nk * quarters
    code_h, code_t = up(n_blk * wide_h, LANES), up(n_blk * wide_t, LANES)
    code_y = up(n_grp * wide_t, LANES)
    slots = up(wide_t, 16) + wide_h
    pairs = n_blk // 2
    hbm = pl.BlockSpec(memory_space=pltpu.HBM)
    vmem = pl.BlockSpec(memory_space=pltpu.VMEM)

    def lanes(values):
        return values.reshape(-1, LANES)

    x, y, weight = pl.pallas_call(
        functools.partial(kernel, n_blk, n_grp),
        out_shape=(
            jax.ShapeDtypeStruct((own_x, LANES), F32),
            jax.ShapeDtypeStruct((own_y, LANES), F32),
            jax.ShapeDtypeStruct((8, LANES), F32),
        ),
        in_specs=[hbm] * 13,
        out_specs=(vmem, vmem, vmem),
        scratch_shapes=[
            pltpu.VMEM((nk + nq, tile, tile), F32),
            pltpu.VMEM((own_x, LANES), jnp.int32),
            pltpu.VMEM((own_y, LANES), jnp.int32),
            pltpu.SMEM((2, nq), jnp.int32),
            pltpu.SMEM((1, nk), jnp.int32),
            pltpu.SMEM((1, nk), jnp.int32),
            pltpu.VMEM((2, n_blk, own_x // 2, LANES), F32),
            pltpu.VMEM((n_grp * own_y, LANES), F32),
            pltpu.VMEM((own_x + slots, LANES), F32),
            pltpu.VMEM((3, 2 * own_x, LANES), F32),
            pltpu.VMEM((3, own_x + slots, LANES), F32),
            pltpu.VMEM((2, n_grp * own_y, LANES), F32),
            pltpu.VMEM((pairs, 3, slots, LANES), F32),
            pltpu.VMEM((pairs, 3, slots, LANES), F32),
            pltpu.VMEM((n_blk, (code_h + code_t) // LANES + 1, LANES), jnp.int32),
            pltpu.VMEM((n_grp, code_y // LANES, LANES), jnp.int32),
            pltpu.VMEM((own_x + slots, code_h), BF16),
            pltpu.VMEM((own_x + slots, code_t), BF16),
            pltpu.VMEM((n_grp * own_y, code_y), BF16),
            pltpu.VMEM((ITERS, n_blk, wide_h, LANES), F32),
            pltpu.VMEM((ITERS, n_blk, wide_t, LANES), F32),
            pltpu.VMEM((ITERS, n_grp, wide_t, LANES), F32),
            pltpu.VMEM((ITERS, n_blk, 1, LANES), F32),
            pltpu.VMEM((ITERS, n_grp, 1, LANES), F32),
            pltpu.VMEM((wide_t, LANES), F32),
            pltpu.SemaphoreType.DMA((2,)),
            pltpu.SemaphoreType.DMA((12,)),
            pltpu.SemaphoreType.DMA((3, pairs)),
            pltpu.SemaphoreType.DMA((9,)),
            pltpu.SemaphoreType.DMA((9,)),
            pltpu.SemaphoreType.DMA((3 * ITERS,)),
            pltpu.SemaphoreType.DMA((3 * ITERS,)),
            pltpu.SemaphoreType.DMA((2 * ITERS + 3,)),
            pltpu.SemaphoreType.DMA((2 * ITERS + 3,)),
        ],
        compiler_params=pltpu.CompilerParams(
            collective_id=0, has_side_effects=True, vmem_limit_bytes=24 * 1024 * 1024
        ),
    )(
        *(
            pltpu.with_memory_space_constraint(item, pltpu.HBM)
            for item in (
                lanes(primal),
                lanes(dual),
                lanes(objective),
                lanes(lower),
                lanes(upper),
                lanes(bound_kind),
                lanes(rhs),
                lanes(row_kind),
                q_index[0],
                k_rows,
                k_cols,
                q_tiles[0],
                k_tiles[0],
            )
        )
    )
    x, y, weight = pl.pallas_call(
        settle,
        out_shape=tuple(jax.ShapeDtypeStruct(shape, F32) for shape in (x.shape, y.shape, (1, 1))),
        in_specs=[vmem] * 3,
        out_specs=(hbm,) * 3,
        scratch_shapes=[pltpu.VMEM((1, 1), F32), pltpu.SemaphoreType.DMA((3,))],
    )(*(pltpu.with_memory_space_constraint(item, pltpu.VMEM) for item in (x, y, weight)))
    return x.reshape(-1), y.reshape(-1), weight.reshape(())


def solution(mesh):
    vector = P(("blk", "grp"))
    return jax.shard_map(
        shards,
        mesh=mesh,
        in_specs=(vector,) * 8
        + (
            P("grp", "blk", None, None),
            P("grp", None, "blk"),
            P("grp", "blk", None, None),
            P("grp", "blk"),
            P("grp", "blk"),
        ),
        out_specs=(vector, vector, P()),
        check_vma=False,
    )
```

```python
import functools
import math

import jax
import jax.numpy as jnp
from jax import lax
from jax.experimental import pallas as pl
from jax.experimental.pallas import tpu as pltpu
from jax.sharding import PartitionSpec as P

ITERS = 2
EPSILON = 1e-06
STEP_SCALE = 0.5
LANES = 128
UNROLL = 8
FREE = 2.0**100
MESH = pl.DeviceIdType.MESH
F32 = jnp.float32
BF16 = jnp.bfloat16


def up(value, step):
    return -(-value // step) * step


def split(values, count=2):
    parts = []
    for _ in range(count):
        parts.append(values.astype(BF16))
        values = values - parts[-1].astype(F32)
    return parts


def partner(me, k, count):
    if count & (count - 1):
        return lax.rem(me + k, count)
    result = 0
    bit = 1
    while bit < count:
        mine, theirs = lax.rem(lax.div(me, bit), 2), lax.rem(lax.div(jnp.int32(k), bit), 2)
        result = result + lax.rem(mine + theirs, 2) * bit
        bit *= 2
    return result


def repeat(first, count, call):
    if count <= UNROLL:
        for k in range(first, count):
            call(k)
    else:

        def body(k, carry):
            call(k)
            return carry

        lax.fori_loop(first, count, body, 0)


def segment(ids, start, width, rows, quarters):
    place = lax.broadcasted_iota(jnp.int32, (rows, LANES), 0) * LANES
    place = place + lax.broadcasted_iota(jnp.int32, (rows, LANES), 1) - start
    result = jnp.full((rows, LANES), -1, jnp.int32)
    for p, tile_id in enumerate(ids):
        for q in range(quarters):
            result = jnp.where(place == p * quarters + q, tile_id * quarters + q, result)
    return jnp.where((place >= 0) & (place < width), result, 0)


def kernel(
    n_blk,
    n_grp,
    primal,
    dual,
    objective,
    lower,
    upper,
    bound_kind,
    rhs,
    row_kind,
    q_index,
    k_rows,
    k_cols,
    q_tiles,
    k_tiles,
    x_out,
    y_out,
    w_out,
    raw,
    kinds,
    row_kinds,
    q_at,
    r_at,
    c_at,
    xs,
    ys,
    xw,
    both,
    data,
    rows_data,
    slot_out,
    slot_in,
    ids_x,
    ids_y,
    sel_h,
    sel_t,
    sel_y,
    vals_h,
    vals_t,
    vals_y,
    sums_x,
    sums_y,
    cons_now,
    tile_sem,
    io_sem,
    far_recv,
    one_recv,
    blk_recv,
    grp_recv,
    y_send,
    all_send,
    spare,
):
    blk, grp = lax.axis_index("blk"), lax.axis_index("grp")
    nq, nk = q_tiles.shape[0], k_tiles.shape[0]
    quarters = q_tiles.shape[-1] // LANES
    own_x, own_y = primal.shape[0], dual.shape[0]
    half_x = own_x // 2
    wide_h, wide_t = nq * quarters, nk * quarters
    pairs = n_blk // 2
    outer, inner = lax.div(blk, 2), lax.rem(blk, 2)
    beside = outer * 2 + 1 - inner
    code_h, code_t = sel_h.shape[1] // LANES, sel_t.shape[1] // LANES
    q_first = up(wide_t, 16)
    first_k, first_q = own_x, own_x + q_first
    last = first_q + wide_h

    barrier = pltpu.get_barrier_semaphore()

    def greet(axis, count, me):
        def one(k):
            pl.semaphore_signal(
                barrier,
                inc=1,
                device_id={axis: partner(me, k, count)},
                device_id_type=MESH,
            )

        repeat(1, count, one)

    greet("blk", n_blk, blk)
    greet("grp", n_grp, grp)

    def part(index, size):
        return pl.ds(pl.multiple_of(index * size, size), size)

    fetched = []
    mine_pair = part(inner, own_x)
    for at, (source, target) in enumerate(
        (
            (dual, ys.at[part(grp, own_y)]),
            (primal.at[:half_x], xs.at[0, blk]),
            (primal.at[half_x:], xs.at[1, blk]),
            (q_index, q_at),
            (k_rows, r_at),
            (k_cols, c_at),
            (bound_kind, kinds),
            (rhs, rows_data.at[0, part(grp, own_y)]),
            (row_kind, row_kinds),
            (objective, both.at[0, mine_pair]),
            (lower, both.at[1, mine_pair]),
            (upper, both.at[2, mine_pair]),
        )
    ):
        fetched.append(pltpu.make_async_copy(source, target, io_sem.at[at]))
        fetched[-1].start()
    for item in fetched:
        item.wait()
    for t in range(nk):
        pltpu.make_async_copy(k_tiles.at[t], raw.at[t], tile_sem.at[0]).start()
    for t in range(nq):
        pltpu.make_async_copy(q_tiles.at[t], raw.at[nk + t], tile_sem.at[1]).start()

    q_rows = [q_at[0, p] for p in range(nq)]
    q_cols = [q_at[1, p] for p in range(nq)]
    c_rows = [r_at[0, p] for p in range(nk)]
    c_cols = [c_at[0, p] for p in range(nk)]
    gap = [-1] * ((q_first - wide_t) // quarters)
    listed = c_cols + gap + q_cols + q_rows
    ids_x[blk] = segment(listed, 0, len(listed) * quarters, 1, quarters)
    ids_y[grp] = segment(c_rows, grp * wide_t, wide_t, ids_y.shape[1], quarters)
    kind = kinds[...]
    both[1, mine_pair] = jnp.where((kind == 1) | (kind == 2), both[1, mine_pair], -FREE)
    both[2, mine_pair] = jnp.where((kind == 2) | (kind == 3), both[2, mine_pair], FREE)
    rows_data[1, part(grp, own_y)] = jnp.where(row_kinds[...] == 1, 0.0, -FREE)

    pl.semaphore_wait(barrier, n_blk + n_grp - 2)

    sent = []
    used = {"blk": 0, "grp": 0, "one": 0}

    def waiter(ref, sem):
        return lambda: pltpu.make_async_copy(ref, ref, sem).wait()

    def send(axis, peer, source, target, send_sem, recv_sem):
        pltpu.make_async_remote_copy(
            src_ref=source,
            dst_ref=target,
            send_sem=send_sem,
            recv_sem=recv_sem,
            device_id={axis: peer},
            device_id_type=MESH,
        ).start()

    def leaves(ref, times):
        sent.append(math.prod(ref.shape[:-1]) * times)

    def channel(axis, others, leave=all_send):
        at = used[axis]
        used[axis] += 1
        count, me = (n_blk, blk) if axis == "blk" else (n_grp, grp)
        recvs = blk_recv if axis == "blk" else grp_recv
        if leave is all_send:
            leaves(others, 1)

        def post(mine):
            repeat(
                1,
                count,
                lambda k: send(
                    axis, partner(me, count - k, count), mine, mine, leave.at[0], recvs.at[at]
                ),
            )

        return post, waiter(others, recvs.at[at])

    def share(axis, mine, others, leave=all_send):
        post, here = channel(axis, others, leave)
        post(mine)
        return here

    def single():
        used["one"] += 1
        return one_recv.at[used["one"] - 1]

    y_rest = ys.at[: (n_grp - 1) * own_y]
    y_here = share("grp", ys.at[part(grp, own_y)], y_rest, y_send)
    ids_x_here = share("blk", ids_x.at[blk], ids_x.at[: n_blk - 1])

    def column(ref, recvs):
        near_recv = single()
        leaves(ref.at[0], 2 * pairs - 1)

        def far():
            def one(k):
                there = partner(outer, pairs - k, pairs) * 2 + inner
                send("blk", there, ref.at[blk], ref.at[blk], all_send.at[0], recvs.at[outer])

            repeat(1, pairs, one)

        def near():
            send("blk", beside, ref.at[blk], ref.at[blk], all_send.at[0], near_recv)

        def relay(k):
            there = partner(outer, k, pairs)
            source = ref.at[there * 2 + inner]
            waiter(source, recvs.at[there])()
            send("blk", beside, source, source, all_send.at[0], near_recv)

        return far, near, relay, waiter(ref.at[:pairs], near_recv)

    lots = [column(xs.at[half], far_recv.at[half]) for half in range(xs.shape[0])]
    for x_far, _, _, _ in lots:
        x_far()

    planes_recv = single()
    planes = both.at[:, mine_pair]
    send("blk", beside, planes, planes, all_send.at[0], planes_recv)
    planes_here = waiter(planes, planes_recv)
    leaves(planes, 1)
    for _, x_near, _, _ in lots:
        x_near()

    ids_y_here = share("grp", ids_y.at[grp], ids_y.at[: n_grp - 1])
    rows_here = share(
        "grp", rows_data.at[:, part(grp, own_y)], rows_data.at[:, : (n_grp - 1) * own_y]
    )

    xw[:half_x] = xs[0, blk]
    xw[half_x:own_x] = xs[1, blk]
    data[:, :own_x] = both[:, mine_pair]
    xw[first_k + wide_t : first_q] = jnp.zeros((q_first - wide_t, LANES), F32)
    data[:, first_k + wide_t : first_q] = jnp.zeros((3, q_first - wide_t, LANES), F32)

    def folded(values):
        return jnp.sum(values.reshape(-1, 8, LANES), axis=0)

    def strip(vector, first, q):
        return jnp.broadcast_to(vector[pl.ds(first + q, 1), :], (LANES, LANES))

    def block(t, q, c):
        return raw[t, q * LANES : (q + 1) * LANES, c * LANES : (c + 1) * LANES]

    def product(vector, first, t, transposed):
        if transposed:
            total = [jnp.zeros((8, LANES), F32)] * quarters
            for q in range(quarters):
                column = strip(vector, first, q).T
                for c in range(quarters):
                    total[c] = total[c] + folded(block(t, q, c) * column)
        else:
            rows = [strip(vector, first, c) for c in range(quarters)]
            total = []
            for q in range(quarters):
                piece = block(t, q, 0) * rows[0]
                for c in range(1, quarters):
                    piece = piece + block(t, q, c) * rows[c]
                total.append(folded(piece.T))
        return [jnp.sum(piece, axis=0, keepdims=True) for piece in total]

    def computed(count, mine, post, one):
        for p in range(count):
            one(p)
        post(mine)

    def transpose_one(step, p):
        for q, piece in enumerate(product(ys, c_rows[p] * quarters, p, True)):
            vals_t[step, blk, pl.ds(p * quarters + q, 1), :] = -piece

    def transposed(step):
        post, here = channel("blk", vals_t.at[step, : n_blk - 1])
        computed(nk, vals_t.at[step, blk], post, lambda p: transpose_one(step, p))
        return here

    def hessian(step):
        post, here = channel("blk", vals_h.at[step, : n_blk - 1])

        def one(p):
            for q, piece in enumerate(product(xw, first_q + p * quarters, nk + p, False)):
                vals_h[step, blk, pl.ds(p * quarters + q, 1), :] = piece

        computed(nq, vals_h.at[step, blk], post, one)
        return here

    def constraint_one(p, call):
        for q, piece in enumerate(product(xw, first_k + p * quarters, p, False)):
            call(pl.ds(p * quarters + q, 1), piece)

    def constraint(step):
        post, here = channel("grp", vals_y.at[step, : n_grp - 1])

        def put(at, piece):
            vals_y[step, grp, at, :] = 2.0 * piece - cons_now[at, :]
            if step < ITERS - 1:
                cons_now[at, :] = piece

        computed(nk, vals_y.at[step, grp], post, lambda p: constraint_one(p, put))
        return here

    def spread(axis, ref, step, value):
        me, count = (blk, n_blk) if axis == "blk" else (grp, n_grp)
        ref[step, me] = jnp.broadcast_to(value, (1, LANES))
        return share(axis, ref.at[step, me], ref.at[step, : count - 1])

    def parts(values):
        return jnp.concatenate(split(values), axis=1)

    def gathered(*terms):
        total = sum(
            jnp.dot(selector, values, preferred_element_type=F32) for selector, values in terms
        )
        return total[:, :LANES] + total[:, LANES:]

    def scalar_sum(ref, step, count):
        total = ref[step, 0]
        for s in range(1, count):
            total = total + ref[step, s]
        return total

    def full_sum(values):
        return jnp.sum(jnp.sum(values, axis=0, keepdims=True), axis=1, keepdims=True)

    def selector(ref, place, codes):
        for k in range(ref.shape[1] // LANES):
            ref[:, k * LANES : (k + 1) * LANES] = jnp.where(
                place == codes[k : k + 1, :], 1.0, 0.0
            ).astype(BF16)

    def lined_up(first, width, rows):
        place = lax.broadcasted_iota(jnp.int32, (rows, LANES), 0) * LANES
        place = place + lax.broadcasted_iota(jnp.int32, (rows, LANES), 1)
        result = jnp.zeros((rows, LANES), jnp.int32)
        for s in range(n_blk):
            moved = pltpu.roll(ids_x[s], (s * width - first) % LANES, 1)
            inside = (place >= s * width) & (place < (s + 1) * width)
            result = jnp.where(inside, jnp.broadcast_to(moved, (rows, LANES)), result)
        return result

    def selectors():
        ids_y_here()
        line = lax.broadcasted_iota(jnp.int32, (last, LANES), 0)
        place = jnp.where(line < own_x, line + blk * own_x, -1)
        for ids, first in ((c_cols, first_k), (q_cols, first_q)):
            for p, tile_id in enumerate(ids):
                begin = first + p * quarters
                inside = (line >= begin) & (line < begin + quarters)
                place = jnp.where(inside, line - begin + tile_id * quarters, place)
        selector(sel_h, place, lined_up(q_first + wide_h, wide_h, code_h))
        selector(sel_t, place, lined_up(0, wide_t, code_t))
        line = lax.broadcasted_iota(jnp.int32, (sel_y.shape[0], LANES), 0)
        selector(sel_y, line, jnp.sum(ids_y[...], axis=0))

    def picked():
        values = jnp.concatenate(
            [piece for plane in range(3) for piece in split(both[plane], 3)], axis=1
        )
        line = lax.broadcasted_iota(jnp.int32, (2 * own_x, LANES), 0) + outer * (2 * own_x)

        def one(k):
            there = partner(outer, k, pairs)
            codes = ids_x[there * 2 + inner]
            hits = jnp.where(line == codes, 1.0, 0.0).T[: slot_out.shape[2]].astype(BF16)
            taken = jnp.dot(hits, values, preferred_element_type=F32)
            for plane in range(3):
                pieces = [
                    taken[:, (plane * 3 + i) * LANES : (plane * 3 + i + 1) * LANES]
                    for i in range(3)
                ]
                slot_out[there, plane] = pieces[0] + (pieces[1] + pieces[2])

        repeat(0, pairs, one)

    def hand_out(first, width):
        recv_sem = single()

        def one(k):
            there = partner(outer, pairs - k, pairs)
            send(
                "blk",
                there * 2 + inner,
                slot_out.at[there, :, first : first + width],
                slot_in.at[outer, :, first : first + width],
                all_send.at[0],
                recv_sem,
            )

        repeat(1, pairs, one)
        whole = slot_in.at[: pairs - 1, :, first : first + width]
        leaves(whole, 1)
        here = waiter(whole, recv_sem)

        def take():
            here()
            total = slot_out[outer, :, first : first + width]
            if pairs <= UNROLL:
                for k in range(1, pairs):
                    total = total + slot_in[partner(outer, k, pairs), :, first : first + width]
            else:
                total = lax.fori_loop(
                    1,
                    pairs,
                    lambda k, so_far: so_far
                    + slot_in[partner(outer, k, pairs), :, first : first + width],
                    total,
                )
            data[:, own_x + first : own_x + first + width] = total

        return take

    def primal_step(step, tau, first, end):
        at = slice(first, end)
        gradient = gathered(
            (sel_h[at, : n_blk * wide_h], parts(vals_h[step].reshape(n_blk * wide_h, LANES))),
            (sel_t[at, : n_blk * wide_t], parts(vals_t[step].reshape(n_blk * wide_t, LANES))),
        )
        gradient = gradient + data[0, at]
        now = xw[at]
        new = jnp.minimum(jnp.maximum(now - tau * gradient, data[1, at]), data[2, at])
        xw[at] = new
        return (new - now) * (new - now)

    def dual_step(step, sigma):
        extrap = gathered((sel_y[:, : n_grp * wide_t], parts(vals_y[step].reshape(n_grp * wide_t, LANES))))
        now = ys[...]
        new = jnp.maximum(now + sigma * (rows_data[0] - extrap), rows_data[1])
        ys[...] = new
        return full_sum((new - now) * (new - now))

    weight = jnp.ones((1, 1), F32)
    repeat(1, pairs, lots[0][2])
    waiter(raw.at[:nk], tile_sem.at[0])()
    y_here()
    for p in range(nk):
        transpose_one(0, p)
    t_far, t_near, t_relay, transposed_here = column(vals_t.at[0], far_recv.at[2])
    t_far()
    repeat(1, pairs, lots[1][2])
    t_near()
    planes_here()
    ids_x_here()
    picked()
    take_k = hand_out(0, wide_t)
    selectors()
    waiter(raw.at[nk:], tile_sem.at[1])()
    lots[0][3]()
    lots[1][3]()
    for ids, first in ((q_cols, first_q), (c_cols, first_k)):
        for p, tile_id in enumerate(ids):
            begin = first + p * quarters
            piece = lax.div(tile_id * quarters, half_x)
            at = lax.rem(tile_id * quarters, half_x)
            xw[begin : begin + quarters] = xs[
                lax.rem(piece, 2), lax.div(piece, 2), pl.ds(at, quarters)
            ]
    hessian_here = hessian(0)
    repeat(1, pairs, t_relay)

    def keep(at, piece):
        cons_now[at, :] = piece

    for p in range(nk):
        constraint_one(p, keep)
    take_q = hand_out(q_first, wide_h)
    take_k()
    for step in range(ITERS):
        hessian_here()
        transposed_here()
        if step > 0:
            dual_here()
            total = scalar_sum(sums_x, step - 1, n_blk)
            ratio = (total[:, :1] + EPSILON) / (total[:, LANES // 2 : LANES // 2 + 1] + EPSILON)
            weight = jnp.sqrt(weight * jnp.sqrt(ratio))
        tau = STEP_SCALE / weight
        moved = full_sum(primal_step(step, tau, 0, first_q)[:own_x])
        constraint_here = constraint(step)
        primal_here = spread("grp", sums_y, step, moved)
        if step < ITERS - 1:
            take_q()
            primal_step(step, tau, first_q, last)
            hessian_here = hessian(step + 1)
        else:
            x_out[...] = xw[:own_x]
        if step == 0:
            rows_here()
            waiter(y_rest, y_send.at[0])()
        constraint_here()
        gone = dual_step(step, STEP_SCALE * weight)
        primal_here()
        lane = lax.broadcasted_iota(jnp.int32, (1, LANES), 1)
        moved = jnp.where(lane < LANES // 2, gone, scalar_sum(sums_y, step, n_grp))
        dual_here = spread("blk", sums_x, step, moved)
        if step < ITERS - 1:
            transposed_here = transposed(step + 1)
    y_out[...] = ys[part(grp, own_y)]
    dual_here()
    total = scalar_sum(sums_x, ITERS - 1, n_blk)
    ratio = (total[:, :1] + EPSILON) / (total[:, LANES // 2 : LANES // 2 + 1] + EPSILON)
    w_out[...] = jnp.broadcast_to(jnp.sqrt(weight * jnp.sqrt(ratio)), w_out.shape)
    waiter(spare.at[: sum(sent)], all_send.at[0])()


def settle(x, y, weight, x_out, y_out, w_out, single, sems):
    single[...] = weight[:1, :1]
    copies = [
        pltpu.make_async_copy(source, target, sems.at[at])
        for at, (source, target) in enumerate(((x, x_out), (y, y_out), (single, w_out)))
    ]
    for copy in copies:
        copy.start()
    for copy in copies:
        copy.wait()


def shards(
    primal,
    dual,
    objective,
    lower,
    upper,
    bound_kind,
    rhs,
    row_kind,
    q_tiles,
    q_index,
    k_tiles,
    k_rows,
    k_cols,
):
    n_blk, n_grp = lax.axis_size("blk"), lax.axis_size("grp")
    nq, nk, tile = q_tiles.shape[1], k_tiles.shape[1], q_tiles.shape[-1]
    quarters = tile // LANES
    own_x, own_y = primal.shape[0] // LANES, dual.shape[0] // LANES
    wide_h, wide_t = nq * quarters, nk * quarters
    code_h, code_t = up(n_blk * wide_h, LANES), up(n_blk * wide_t, LANES)
    code_y = up(n_grp * wide_t, LANES)
    slots = up(wide_t, 16) + wide_h
    pairs = n_blk // 2
    sent = (n_blk - 1) * (1 + (ITERS - 1) * wide_t + ITERS * (wide_h + 1))
    sent += (n_grp - 1) * (code_y // LANES + 2 * own_y + ITERS * (wide_t + 1))
    sent += (2 * pairs - 1) * (own_x + wide_t) + 3 * own_x
    sent += (pairs - 1) * 3 * (wide_t + wide_h)
    hbm = pl.BlockSpec(memory_space=pltpu.HBM)
    vmem = pl.BlockSpec(memory_space=pltpu.VMEM)

    def lanes(values):
        return values.reshape(-1, LANES)

    x, y, weight = pl.pallas_call(
        functools.partial(kernel, n_blk, n_grp),
        out_shape=(
            jax.ShapeDtypeStruct((own_x, LANES), F32),
            jax.ShapeDtypeStruct((own_y, LANES), F32),
            jax.ShapeDtypeStruct((8, LANES), F32),
        ),
        in_specs=[hbm] * 13,
        out_specs=(vmem, vmem, vmem),
        scratch_shapes=[
            pltpu.VMEM((nk + nq, tile, tile), F32),
            pltpu.VMEM((own_x, LANES), jnp.int32),
            pltpu.VMEM((own_y, LANES), jnp.int32),
            pltpu.SMEM((2, nq), jnp.int32),
            pltpu.SMEM((1, nk), jnp.int32),
            pltpu.SMEM((1, nk), jnp.int32),
            pltpu.VMEM((2, n_blk, own_x // 2, LANES), F32),
            pltpu.VMEM((n_grp * own_y, LANES), F32),
            pltpu.VMEM((own_x + slots, LANES), F32),
            pltpu.VMEM((3, 2 * own_x, LANES), F32),
            pltpu.VMEM((3, own_x + slots, LANES), F32),
            pltpu.VMEM((2, n_grp * own_y, LANES), F32),
            pltpu.VMEM((pairs, 3, slots, LANES), F32),
            pltpu.VMEM((pairs, 3, slots, LANES), F32),
            pltpu.VMEM((n_blk, 1, LANES), jnp.int32),
            pltpu.VMEM((n_grp, code_y // LANES, LANES), jnp.int32),
            pltpu.VMEM((own_x + slots, code_h), BF16),
            pltpu.VMEM((own_x + slots, code_t), BF16),
            pltpu.VMEM((n_grp * own_y, code_y), BF16),
            pltpu.VMEM((ITERS, n_blk, wide_h, LANES), F32),
            pltpu.VMEM((ITERS, n_blk, wide_t, LANES), F32),
            pltpu.VMEM((ITERS, n_grp, wide_t, LANES), F32),
            pltpu.VMEM((ITERS, n_blk, 1, LANES), F32),
            pltpu.VMEM((ITERS, n_grp, 1, LANES), F32),
            pltpu.VMEM((wide_t, LANES), F32),
            pltpu.SemaphoreType.DMA((2,)),
            pltpu.SemaphoreType.DMA((12,)),
            pltpu.SemaphoreType.DMA((3, pairs)),
            pltpu.SemaphoreType.DMA((6,)),
            pltpu.SemaphoreType.DMA((3 * ITERS,)),
            pltpu.SemaphoreType.DMA((2 * ITERS + 3,)),
            pltpu.SemaphoreType.DMA((1,)),
            pltpu.SemaphoreType.DMA((1,)),
            pltpu.VMEM((sent, LANES), F32),
        ],
        compiler_params=pltpu.CompilerParams(
            collective_id=0, has_side_effects=True, vmem_limit_bytes=40 * 1024 * 1024
        ),
    )(
        *(
            pltpu.with_memory_space_constraint(item, pltpu.HBM)
            for item in (
                lanes(primal),
                lanes(dual),
                lanes(objective),
                lanes(lower),
                lanes(upper),
                lanes(bound_kind),
                lanes(rhs),
                lanes(row_kind),
                q_index[0],
                k_rows,
                k_cols,
                q_tiles[0],
                k_tiles[0],
            )
        )
    )
    x, y, weight = pl.pallas_call(
        settle,
        out_shape=tuple(jax.ShapeDtypeStruct(shape, F32) for shape in (x.shape, y.shape, (1, 1))),
        in_specs=[vmem] * 3,
        out_specs=(hbm,) * 3,
        scratch_shapes=[pltpu.VMEM((1, 1), F32), pltpu.SemaphoreType.DMA((3,))],
    )(*(pltpu.with_memory_space_constraint(item, pltpu.VMEM) for item in (x, y, weight)))
    return x.reshape(-1), y.reshape(-1), weight.reshape(())


def solution(mesh):
    vector = P(("blk", "grp"))
    return jax.shard_map(
        shards,
        mesh=mesh,
        in_specs=(vector,) * 8
        + (
            P("grp", "blk", None, None),
            P("grp", None, "blk"),
            P("grp", "blk", None, None),
            P("grp", "blk"),
            P("grp", "blk"),
        ),
        out_specs=(vector, vector, P()),
        check_vma=False,
    )
```

```python
import functools
import math

import jax
import jax.numpy as jnp
from jax import lax
from jax.experimental import pallas as pl
from jax.experimental.pallas import tpu as pltpu
from jax.sharding import PartitionSpec as P

ITERS = 2
EPSILON = 1e-06
STEP_SCALE = 0.5
LANES = 128
UNROLL = 8
FREE = 2.0**100
MESH = pl.DeviceIdType.MESH
F32 = jnp.float32
BF16 = jnp.bfloat16


def up(value, step):
    return -(-value // step) * step


def split(values, count=2):
    parts = []
    for _ in range(count):
        parts.append(values.astype(BF16))
        values = values - parts[-1].astype(F32)
    return parts


def partner(me, k, count):
    if count & (count - 1):
        return lax.rem(me + k, count)
    result = 0
    bit = 1
    while bit < count:
        mine, theirs = lax.rem(lax.div(me, bit), 2), lax.rem(lax.div(jnp.int32(k), bit), 2)
        result = result + lax.rem(mine + theirs, 2) * bit
        bit *= 2
    return result


def farthest(me, j, count):
    upper = lax.div(me, (count + 1) // 2)
    from_top = count - 1 - j - lax.div(me + j, count - 1)
    from_bottom = j + lax.div(j + count - me, count)
    return from_top + upper * (from_bottom - from_top)


def repeat(first, count, call):
    if count <= UNROLL:
        for k in range(first, count):
            call(k)
    else:

        def body(k, carry):
            call(k)
            return carry

        lax.fori_loop(first, count, body, 0)


def segment(ids, start, width, rows, quarters):
    place = lax.broadcasted_iota(jnp.int32, (rows, LANES), 0) * LANES
    place = place + lax.broadcasted_iota(jnp.int32, (rows, LANES), 1) - start
    result = jnp.full((rows, LANES), -1, jnp.int32)
    for p, tile_id in enumerate(ids):
        for q in range(quarters):
            result = jnp.where(place == p * quarters + q, tile_id * quarters + q, result)
    return jnp.where((place >= 0) & (place < width), result, 0)


def kernel(
    n_blk,
    n_grp,
    primal,
    dual,
    objective,
    lower,
    upper,
    bound_kind,
    rhs,
    row_kind,
    q_index,
    k_rows,
    k_cols,
    q_tiles,
    k_tiles,
    x_out,
    y_out,
    w_out,
    raw,
    kinds,
    row_kinds,
    q_at,
    r_at,
    c_at,
    xs,
    ys,
    xw,
    both,
    data,
    rows_data,
    slot_out,
    slot_in,
    ids_x,
    ids_y,
    sel_h,
    sel_t,
    sel_y,
    vals_h,
    vals_t,
    vals_y,
    sums_x,
    sums_y,
    cons_now,
    tile_sem,
    io_sem,
    far_recv,
    one_recv,
    blk_recv,
    grp_recv,
    y_send,
    all_send,
    spare,
):
    blk, grp = lax.axis_index("blk"), lax.axis_index("grp")
    nq, nk = q_tiles.shape[0], k_tiles.shape[0]
    quarters = q_tiles.shape[-1] // LANES
    own_x, own_y = primal.shape[0], dual.shape[0]
    half_x = own_x // 2
    wide_h, wide_t = nq * quarters, nk * quarters
    pairs = n_blk // 2
    outer, inner = lax.div(blk, 2), lax.rem(blk, 2)
    beside = outer * 2 + 1 - inner
    code_h, code_t = sel_h.shape[1] // LANES, sel_t.shape[1] // LANES
    q_first = up(wide_t, 16)
    first_k, first_q = own_x, own_x + q_first
    last = first_q + wide_h

    barrier = pltpu.get_barrier_semaphore()

    def greet(axis, count, me):
        def one(k):
            pl.semaphore_signal(
                barrier,
                inc=1,
                device_id={axis: partner(me, k, count)},
                device_id_type=MESH,
            )

        repeat(1, count, one)

    greet("blk", n_blk, blk)
    greet("grp", n_grp, grp)

    def part(index, size):
        return pl.ds(pl.multiple_of(index * size, size), size)

    fetched = []
    mine_pair = part(inner, own_x)
    for at, (source, target) in enumerate(
        (
            (dual, ys.at[part(grp, own_y)]),
            (primal.at[:half_x], xs.at[0, blk]),
            (primal.at[half_x:], xs.at[1, blk]),
            (q_index, q_at),
            (k_rows, r_at),
            (k_cols, c_at),
            (bound_kind, kinds),
            (rhs, rows_data.at[0, part(grp, own_y)]),
            (row_kind, row_kinds),
            (objective, both.at[0, mine_pair]),
            (lower, both.at[1, mine_pair]),
            (upper, both.at[2, mine_pair]),
        )
    ):
        fetched.append(pltpu.make_async_copy(source, target, io_sem.at[at]))
        fetched[-1].start()
    for item in fetched:
        item.wait()
    for t in range(nk):
        pltpu.make_async_copy(k_tiles.at[t], raw.at[t], tile_sem.at[0]).start()
    for t in range(nq):
        pltpu.make_async_copy(q_tiles.at[t], raw.at[nk + t], tile_sem.at[1]).start()

    q_rows = [q_at[0, p] for p in range(nq)]
    q_cols = [q_at[1, p] for p in range(nq)]
    c_rows = [r_at[0, p] for p in range(nk)]
    c_cols = [c_at[0, p] for p in range(nk)]
    gap = [-1] * ((q_first - wide_t) // quarters)
    listed = c_cols + gap + q_cols + q_rows
    ids_x[blk] = segment(listed, 0, len(listed) * quarters, 1, quarters)
    ids_y[grp] = segment(c_rows, grp * wide_t, wide_t, ids_y.shape[1], quarters)
    kind = kinds[...]
    both[1, mine_pair] = jnp.where((kind == 1) | (kind == 2), both[1, mine_pair], -FREE)
    both[2, mine_pair] = jnp.where((kind == 2) | (kind == 3), both[2, mine_pair], FREE)
    rows_data[1, part(grp, own_y)] = jnp.where(row_kinds[...] == 1, 0.0, -FREE)

    pl.semaphore_wait(barrier, n_blk + n_grp - 2)

    sent = []
    used = {"blk": 0, "grp": 0, "one": 0}

    def waiter(ref, sem):
        return lambda: pltpu.make_async_copy(ref, ref, sem).wait()

    def send(axis, peer, source, target, send_sem, recv_sem):
        pltpu.make_async_remote_copy(
            src_ref=source,
            dst_ref=target,
            send_sem=send_sem,
            recv_sem=recv_sem,
            device_id={axis: peer},
            device_id_type=MESH,
        ).start()

    def leaves(ref, times):
        sent.append(math.prod(ref.shape[:-1]) * times)

    def channel(axis, others, leave=all_send):
        at = used[axis]
        used[axis] += 1
        count, me = (n_blk, blk) if axis == "blk" else (n_grp, grp)
        recvs = blk_recv if axis == "blk" else grp_recv
        if leave is all_send:
            leaves(others, 1)

        def post(mine):
            repeat(
                1,
                count,
                lambda k: send(
                    axis, farthest(me, k - 1, count), mine, mine, leave.at[0], recvs.at[at]
                ),
            )

        return post, waiter(others, recvs.at[at])

    def share(axis, mine, others, leave=all_send):
        post, here = channel(axis, others, leave)
        post(mine)
        return here

    def single():
        used["one"] += 1
        return one_recv.at[used["one"] - 1]

    y_rest = ys.at[: (n_grp - 1) * own_y]
    y_here = share("grp", ys.at[part(grp, own_y)], y_rest, y_send)
    ids_x_here = share("blk", ids_x.at[blk], ids_x.at[: n_blk - 1])

    def column(ref, recvs):
        near_recv = single()
        leaves(ref.at[0], 2 * pairs - 1)

        def far():
            def one(k):
                there = farthest(outer, k - 1, pairs) * 2 + inner
                send("blk", there, ref.at[blk], ref.at[blk], all_send.at[0], recvs.at[outer])

            repeat(1, pairs, one)

        def near():
            send("blk", beside, ref.at[blk], ref.at[blk], all_send.at[0], near_recv)

        def relay(k):
            there = partner(outer, k, pairs)
            source = ref.at[there * 2 + inner]
            waiter(source, recvs.at[there])()
            send("blk", beside, source, source, all_send.at[0], near_recv)

        return far, near, relay, waiter(ref.at[:pairs], near_recv)

    lots = [column(xs.at[half], far_recv.at[half]) for half in range(xs.shape[0])]
    for x_far, _, _, _ in lots:
        x_far()

    planes_recv = single()
    planes = both.at[:, mine_pair]
    send("blk", beside, planes, planes, all_send.at[0], planes_recv)
    planes_here = waiter(planes, planes_recv)
    leaves(planes, 1)
    for _, x_near, _, _ in lots:
        x_near()

    ids_y_here = share("grp", ids_y.at[grp], ids_y.at[: n_grp - 1])
    rows_here = share(
        "grp", rows_data.at[:, part(grp, own_y)], rows_data.at[:, : (n_grp - 1) * own_y]
    )

    xw[:half_x] = xs[0, blk]
    xw[half_x:own_x] = xs[1, blk]
    data[:, :own_x] = both[:, mine_pair]
    xw[first_k + wide_t : first_q] = jnp.zeros((q_first - wide_t, LANES), F32)
    data[:, first_k + wide_t : first_q] = jnp.zeros((3, q_first - wide_t, LANES), F32)

    def folded(values):
        return jnp.sum(values.reshape(-1, 8, LANES), axis=0)

    def strip(vector, first, q):
        return jnp.broadcast_to(vector[pl.ds(first + q, 1), :], (LANES, LANES))

    def block(t, q, c):
        return raw[t, q * LANES : (q + 1) * LANES, c * LANES : (c + 1) * LANES]

    def product(vector, first, t, transposed):
        if transposed:
            total = [jnp.zeros((8, LANES), F32)] * quarters
            for q in range(quarters):
                column = strip(vector, first, q).T
                for c in range(quarters):
                    total[c] = total[c] + folded(block(t, q, c) * column)
        else:
            rows = [strip(vector, first, c) for c in range(quarters)]
            total = []
            for q in range(quarters):
                piece = block(t, q, 0) * rows[0]
                for c in range(1, quarters):
                    piece = piece + block(t, q, c) * rows[c]
                total.append(folded(piece.T))
        return [jnp.sum(piece, axis=0, keepdims=True) for piece in total]

    def computed(count, mine, post, one):
        for p in range(count):
            one(p)
        post(mine)

    def transpose_one(step, p):
        for q, piece in enumerate(product(ys, c_rows[p] * quarters, p, True)):
            vals_t[step, blk, pl.ds(p * quarters + q, 1), :] = -piece

    def transposed(step):
        post, here = channel("blk", vals_t.at[step, : n_blk - 1])
        computed(nk, vals_t.at[step, blk], post, lambda p: transpose_one(step, p))
        return here

    def hessian(step):
        post, here = channel("blk", vals_h.at[step, : n_blk - 1])

        def one(p):
            for q, piece in enumerate(product(xw, first_q + p * quarters, nk + p, False)):
                vals_h[step, blk, pl.ds(p * quarters + q, 1), :] = piece

        computed(nq, vals_h.at[step, blk], post, one)
        return here

    def constraint_one(p, call):
        for q, piece in enumerate(product(xw, first_k + p * quarters, p, False)):
            call(pl.ds(p * quarters + q, 1), piece)

    def constraint(step):
        post, here = channel("grp", vals_y.at[step, : n_grp - 1])

        def put(at, piece):
            vals_y[step, grp, at, :] = 2.0 * piece - cons_now[at, :]
            if step < ITERS - 1:
                cons_now[at, :] = piece

        computed(nk, vals_y.at[step, grp], post, lambda p: constraint_one(p, put))
        return here

    def spread(axis, ref, step, value):
        me, count = (blk, n_blk) if axis == "blk" else (grp, n_grp)
        ref[step, me] = jnp.broadcast_to(value, (1, LANES))
        return share(axis, ref.at[step, me], ref.at[step, : count - 1])

    def parts(values):
        return jnp.concatenate(split(values), axis=1)

    def gathered(*terms):
        total = sum(
            jnp.dot(selector, values, preferred_element_type=F32) for selector, values in terms
        )
        return total[:, :LANES] + total[:, LANES:]

    def scalar_sum(ref, step, count):
        total = ref[step, 0]
        for s in range(1, count):
            total = total + ref[step, s]
        return total

    def full_sum(values):
        return jnp.sum(jnp.sum(values, axis=0, keepdims=True), axis=1, keepdims=True)

    def selector(ref, place, codes):
        for k in range(ref.shape[1] // LANES):
            ref[:, k * LANES : (k + 1) * LANES] = jnp.where(
                place == codes[k : k + 1, :], 1.0, 0.0
            ).astype(BF16)

    def lined_up(first, width, rows):
        place = lax.broadcasted_iota(jnp.int32, (rows, LANES), 0) * LANES
        place = place + lax.broadcasted_iota(jnp.int32, (rows, LANES), 1)
        result = jnp.zeros((rows, LANES), jnp.int32)
        for s in range(n_blk):
            moved = pltpu.roll(ids_x[s], (s * width - first) % LANES, 1)
            inside = (place >= s * width) & (place < (s + 1) * width)
            result = jnp.where(inside, jnp.broadcast_to(moved, (rows, LANES)), result)
        return result

    def selectors():
        ids_y_here()
        line = lax.broadcasted_iota(jnp.int32, (last, LANES), 0)
        place = jnp.where(line < own_x, line + blk * own_x, -1)
        for ids, first in ((c_cols, first_k), (q_cols, first_q)):
            for p, tile_id in enumerate(ids):
                begin = first + p * quarters
                inside = (line >= begin) & (line < begin + quarters)
                place = jnp.where(inside, line - begin + tile_id * quarters, place)
        selector(sel_h, place, lined_up(q_first + wide_h, wide_h, code_h))
        selector(sel_t, place, lined_up(0, wide_t, code_t))
        line = lax.broadcasted_iota(jnp.int32, (sel_y.shape[0], LANES), 0)
        selector(sel_y, line, jnp.sum(ids_y[...], axis=0))

    def picked():
        values = jnp.concatenate(
            [piece for plane in range(3) for piece in split(both[plane], 3)], axis=1
        )
        line = lax.broadcasted_iota(jnp.int32, (2 * own_x, LANES), 0) + outer * (2 * own_x)

        def one(k):
            there = partner(outer, k, pairs)
            codes = ids_x[there * 2 + inner]
            hits = jnp.where(line == codes, 1.0, 0.0).T[: slot_out.shape[2]].astype(BF16)
            taken = jnp.dot(hits, values, preferred_element_type=F32)
            for plane in range(3):
                pieces = [
                    taken[:, (plane * 3 + i) * LANES : (plane * 3 + i + 1) * LANES]
                    for i in range(3)
                ]
                slot_out[there, plane] = pieces[0] + (pieces[1] + pieces[2])

        repeat(0, pairs, one)

    def hand_out(first, width):
        recv_sem = single()

        def one(k):
            there = farthest(outer, k - 1, pairs)
            send(
                "blk",
                there * 2 + inner,
                slot_out.at[there, :, first : first + width],
                slot_in.at[outer, :, first : first + width],
                all_send.at[0],
                recv_sem,
            )

        repeat(1, pairs, one)
        whole = slot_in.at[: pairs - 1, :, first : first + width]
        leaves(whole, 1)
        here = waiter(whole, recv_sem)

        def take():
            here()
            total = slot_out[outer, :, first : first + width]
            if pairs <= UNROLL:
                for k in range(1, pairs):
                    total = total + slot_in[partner(outer, k, pairs), :, first : first + width]
            else:
                total = lax.fori_loop(
                    1,
                    pairs,
                    lambda k, so_far: so_far
                    + slot_in[partner(outer, k, pairs), :, first : first + width],
                    total,
                )
            data[:, own_x + first : own_x + first + width] = total

        return take

    def primal_step(step, tau, first, end):
        at = slice(first, end)
        gradient = gathered(
            (sel_h[at, : n_blk * wide_h], parts(vals_h[step].reshape(n_blk * wide_h, LANES))),
            (sel_t[at, : n_blk * wide_t], parts(vals_t[step].reshape(n_blk * wide_t, LANES))),
        )
        gradient = gradient + data[0, at]
        now = xw[at]
        new = jnp.minimum(jnp.maximum(now - tau * gradient, data[1, at]), data[2, at])
        xw[at] = new
        return (new - now) * (new - now)

    def dual_step(step, sigma):
        extrap = gathered((sel_y[:, : n_grp * wide_t], parts(vals_y[step].reshape(n_grp * wide_t, LANES))))
        now = ys[...]
        new = jnp.maximum(now + sigma * (rows_data[0] - extrap), rows_data[1])
        ys[...] = new
        return full_sum((new - now) * (new - now))

    weight = jnp.ones((1, 1), F32)
    repeat(1, pairs, lots[0][2])
    waiter(raw.at[:nk], tile_sem.at[0])()
    y_here()
    for p in range(nk):
        transpose_one(0, p)
    t_far, t_near, t_relay, transposed_here = column(vals_t.at[0], far_recv.at[2])
    t_far()
    repeat(1, pairs, lots[1][2])
    t_near()
    planes_here()
    ids_x_here()
    picked()
    take_k = hand_out(0, wide_t)
    selectors()
    waiter(raw.at[nk:], tile_sem.at[1])()
    lots[0][3]()
    lots[1][3]()
    for ids, first in ((q_cols, first_q), (c_cols, first_k)):
        for p, tile_id in enumerate(ids):
            begin = first + p * quarters
            piece = lax.div(tile_id * quarters, half_x)
            at = lax.rem(tile_id * quarters, half_x)
            xw[begin : begin + quarters] = xs[
                lax.rem(piece, 2), lax.div(piece, 2), pl.ds(at, quarters)
            ]
    hessian_here = hessian(0)
    repeat(1, pairs, t_relay)

    def keep(at, piece):
        cons_now[at, :] = piece

    for p in range(nk):
        constraint_one(p, keep)
    take_q = hand_out(q_first, wide_h)
    take_k()
    for step in range(ITERS):
        hessian_here()
        transposed_here()
        if step > 0:
            dual_here()
            total = scalar_sum(sums_x, step - 1, n_blk)
            ratio = (total[:, :1] + EPSILON) / (total[:, LANES // 2 : LANES // 2 + 1] + EPSILON)
            weight = jnp.sqrt(weight * jnp.sqrt(ratio))
        tau = STEP_SCALE / weight
        moved = full_sum(primal_step(step, tau, 0, first_q)[:own_x])
        constraint_here = constraint(step)
        primal_here = spread("grp", sums_y, step, moved)
        if step < ITERS - 1:
            take_q()
            primal_step(step, tau, first_q, last)
            hessian_here = hessian(step + 1)
        else:
            x_out[...] = xw[:own_x]
        if step == 0:
            rows_here()
            waiter(y_rest, y_send.at[0])()
        constraint_here()
        gone = dual_step(step, STEP_SCALE * weight)
        primal_here()
        lane = lax.broadcasted_iota(jnp.int32, (1, LANES), 1)
        moved = jnp.where(lane < LANES // 2, gone, scalar_sum(sums_y, step, n_grp))
        dual_here = spread("blk", sums_x, step, moved)
        if step < ITERS - 1:
            transposed_here = transposed(step + 1)
    y_out[...] = ys[part(grp, own_y)]
    dual_here()
    total = scalar_sum(sums_x, ITERS - 1, n_blk)
    ratio = (total[:, :1] + EPSILON) / (total[:, LANES // 2 : LANES // 2 + 1] + EPSILON)
    w_out[...] = jnp.broadcast_to(jnp.sqrt(weight * jnp.sqrt(ratio)), w_out.shape)
    waiter(spare.at[: sum(sent)], all_send.at[0])()


def settle(x, y, weight, x_out, y_out, w_out, single, sems):
    single[...] = weight[:1, :1]
    copies = [
        pltpu.make_async_copy(source, target, sems.at[at])
        for at, (source, target) in enumerate(((x, x_out), (y, y_out), (single, w_out)))
    ]
    for copy in copies:
        copy.start()
    for copy in copies:
        copy.wait()


def shards(
    primal,
    dual,
    objective,
    lower,
    upper,
    bound_kind,
    rhs,
    row_kind,
    q_tiles,
    q_index,
    k_tiles,
    k_rows,
    k_cols,
):
    n_blk, n_grp = lax.axis_size("blk"), lax.axis_size("grp")
    nq, nk, tile = q_tiles.shape[1], k_tiles.shape[1], q_tiles.shape[-1]
    quarters = tile // LANES
    own_x, own_y = primal.shape[0] // LANES, dual.shape[0] // LANES
    wide_h, wide_t = nq * quarters, nk * quarters
    code_h, code_t = up(n_blk * wide_h, LANES), up(n_blk * wide_t, LANES)
    code_y = up(n_grp * wide_t, LANES)
    slots = up(wide_t, 16) + wide_h
    pairs = n_blk // 2
    sent = (n_blk - 1) * (1 + (ITERS - 1) * wide_t + ITERS * (wide_h + 1))
    sent += (n_grp - 1) * (code_y // LANES + 2 * own_y + ITERS * (wide_t + 1))
    sent += (2 * pairs - 1) * (own_x + wide_t) + 3 * own_x
    sent += (pairs - 1) * 3 * (wide_t + wide_h)
    hbm = pl.BlockSpec(memory_space=pltpu.HBM)
    vmem = pl.BlockSpec(memory_space=pltpu.VMEM)

    def lanes(values):
        return values.reshape(-1, LANES)

    x, y, weight = pl.pallas_call(
        functools.partial(kernel, n_blk, n_grp),
        out_shape=(
            jax.ShapeDtypeStruct((own_x, LANES), F32),
            jax.ShapeDtypeStruct((own_y, LANES), F32),
            jax.ShapeDtypeStruct((8, LANES), F32),
        ),
        in_specs=[hbm] * 13,
        out_specs=(vmem, vmem, vmem),
        scratch_shapes=[
            pltpu.VMEM((nk + nq, tile, tile), F32),
            pltpu.VMEM((own_x, LANES), jnp.int32),
            pltpu.VMEM((own_y, LANES), jnp.int32),
            pltpu.SMEM((2, nq), jnp.int32),
            pltpu.SMEM((1, nk), jnp.int32),
            pltpu.SMEM((1, nk), jnp.int32),
            pltpu.VMEM((2, n_blk, own_x // 2, LANES), F32),
            pltpu.VMEM((n_grp * own_y, LANES), F32),
            pltpu.VMEM((own_x + slots, LANES), F32),
            pltpu.VMEM((3, 2 * own_x, LANES), F32),
            pltpu.VMEM((3, own_x + slots, LANES), F32),
            pltpu.VMEM((2, n_grp * own_y, LANES), F32),
            pltpu.VMEM((pairs, 3, slots, LANES), F32),
            pltpu.VMEM((pairs, 3, slots, LANES), F32),
            pltpu.VMEM((n_blk, 1, LANES), jnp.int32),
            pltpu.VMEM((n_grp, code_y // LANES, LANES), jnp.int32),
            pltpu.VMEM((own_x + slots, code_h), BF16),
            pltpu.VMEM((own_x + slots, code_t), BF16),
            pltpu.VMEM((n_grp * own_y, code_y), BF16),
            pltpu.VMEM((ITERS, n_blk, wide_h, LANES), F32),
            pltpu.VMEM((ITERS, n_blk, wide_t, LANES), F32),
            pltpu.VMEM((ITERS, n_grp, wide_t, LANES), F32),
            pltpu.VMEM((ITERS, n_blk, 1, LANES), F32),
            pltpu.VMEM((ITERS, n_grp, 1, LANES), F32),
            pltpu.VMEM((wide_t, LANES), F32),
            pltpu.SemaphoreType.DMA((2,)),
            pltpu.SemaphoreType.DMA((12,)),
            pltpu.SemaphoreType.DMA((3, pairs)),
            pltpu.SemaphoreType.DMA((6,)),
            pltpu.SemaphoreType.DMA((3 * ITERS,)),
            pltpu.SemaphoreType.DMA((2 * ITERS + 3,)),
            pltpu.SemaphoreType.DMA((1,)),
            pltpu.SemaphoreType.DMA((1,)),
            pltpu.VMEM((sent, LANES), F32),
        ],
        compiler_params=pltpu.CompilerParams(
            collective_id=0, has_side_effects=True, vmem_limit_bytes=40 * 1024 * 1024
        ),
    )(
        *(
            pltpu.with_memory_space_constraint(item, pltpu.HBM)
            for item in (
                lanes(primal),
                lanes(dual),
                lanes(objective),
                lanes(lower),
                lanes(upper),
                lanes(bound_kind),
                lanes(rhs),
                lanes(row_kind),
                q_index[0],
                k_rows,
                k_cols,
                q_tiles[0],
                k_tiles[0],
            )
        )
    )
    x, y, weight = pl.pallas_call(
        settle,
        out_shape=tuple(jax.ShapeDtypeStruct(shape, F32) for shape in (x.shape, y.shape, (1, 1))),
        in_specs=[vmem] * 3,
        out_specs=(hbm,) * 3,
        scratch_shapes=[pltpu.VMEM((1, 1), F32), pltpu.SemaphoreType.DMA((3,))],
    )(*(pltpu.with_memory_space_constraint(item, pltpu.VMEM) for item in (x, y, weight)))
    return x.reshape(-1), y.reshape(-1), weight.reshape(())


def solution(mesh):
    vector = P(("blk", "grp"))
    return jax.shard_map(
        shards,
        mesh=mesh,
        in_specs=(vector,) * 8
        + (
            P("grp", "blk", None, None),
            P("grp", None, "blk"),
            P("grp", "blk", None, None),
            P("grp", "blk"),
            P("grp", "blk"),
        ),
        out_specs=(vector, vector, P()),
        check_vma=False,
    )
```
